128 devices in a mesh: gx: 32 (over z, x, core), gy: 4 (over y).
Axes of the slice: x: 4, y: 4, z: 4, core: 2. Of those that a mesh axis runs over, the one named last changes fastest.
Arguments:
- velocity: float32 [3, 32768, 512], P(None, ('gx', 'gy')), may hold values from -6 to 6
- positions: float32 [3, 4096, 256], P(None, ('gx', 'gy')), may hold values from -6 to 6
- stiff_h: float32 [4096, 256], P(('gx', 'gy')), may hold values from 0.1 to 1
- stiff_v: float32 [4096, 256], P(('gx', 'gy')), may hold values from 0.1 to 1
- marker_owner: int32 [1048576, 1], P(('gx', 'gy')), may hold values from 0 to 127; in each aligned block of 8192 rows (0 to 8191, 8192 to 16383, ...) at most 96 rows name the same one
- marker_element: int32 [1048576], P(('gx', 'gy')), may hold values from 0 to 255
- marker_coords: float32 [3, 1048576], P(None, ('gx', 'gy')), may hold values from -1 to 1
Outputs:
- new_positions: float32 [3, 4096, 256], P(None, ('gx', 'gy'))
- node_forces: float32 [3, 32768, 512], P(None, ('gx', 'gy'))
The draws below stay inside these ranges and needn't reach their ends.
Inputs may be any that keep to these rules, and one draw needn't show every extreme that they name: `marker_owner`: among the markers of one device's rows, no owner is named more than 96 times, and in some devices' rows one owner is named exactly 96 times.
All inputs are finite; a program needn't handle non-finite values.
Results may differ from the reference program's by a relative error of at most 0.00013.
Values sent between devices are 32-bit elements; how exact they have to be, the bound alone decides.
A program may use at most 64 MiB of HBM per device.

```python
import math
import jax
import jax.numpy as jnp
import numpy as np
from jax import lax

POINTS = 8
NODES = 512
E_DEV = 256
ELEMS = 32768
COLS = 256
M_DEV = 8192
ROWS = 4096
MARKERS = 1048576
CAP = 96
DEVICES = 128


def plant(drawn, own_key, low, high):
    dims = drawn.shape
    place = [jax.random.randint(jax.random.fold_in(own_key, axis), (), 0, dims[axis]) for axis in range(len(dims))]
    drawn = drawn.at[tuple(place)].set(low)
    longest = dims.index(max(dims))
    place[longest] = (place[longest] + 1) % dims[longest]
    return drawn.at[tuple(place)].set(high)


def levels(stream_key, shape, split, smallest, top_value):
    def one(axis_at, blocks):
        heights = jax.random.uniform(jax.random.fold_in(jax.random.fold_in(stream_key, 6), axis_at), (blocks,), jnp.float32, smallest / len(split), top_value / len(split))
        return jnp.repeat(jnp.exp(heights), shape[axis_at] // blocks).reshape((-1,) + (1,) * (len(shape) - axis_at - 1))

    level = one(*split[0])
    for cut in split[1:]:
        level = level * one(*cut)
    return level


def assign_block(rng, own, number, rows, amount, top, bound, slope):
    order = jax.random.permutation(rng, amount)
    heavy_load, usual = shares(amount, rows * top, bound, slope, True), shares(amount, rows * top, bound, slope, False)
    places = jnp.arange(amount)

    def named(tallies, rotation):
        used = int((tallies > 0).sum())
        fixed = max(1, used // 4)
        moved = fixed + (places - fixed + rotation * (used - fixed)) % max(1, amount - fixed)
        return jnp.zeros((amount,), jnp.int32).at[order[jnp.where(places < fixed, places, moved)]].set(jnp.asarray(tallies, jnp.int32))

    tallies = jnp.where(number % 4 == 0, named(heavy_load, number // 4), named(usual, number - number // 4 - 1))
    mixed = jax.random.permutation(jax.random.fold_in(own, 3), amount)
    giver, taker = mixed[0:amount // 2 * 2:2], mixed[1:amount // 2 * 2:2]
    slack = jnp.minimum(tallies[giver] - 1, bound - tallies[taker]) // 2
    slack = jnp.where((giver == order[0]) | (taker == order[0]) | (tallies[taker] == 0), 0, jnp.maximum(slack, 0))
    moved = jax.random.randint(jax.random.fold_in(own, 4), (amount // 2,), 0, 1 << 20) % (slack + 1)
    tallies = tallies.at[giver].add(-moved).at[taker].add(moved)
    labels = jnp.searchsorted(jnp.cumsum(tallies), jnp.arange(rows * top), side="right").astype(jnp.int32)
    table = labels.reshape(top, rows).T
    table = table[jax.random.permutation(jax.random.fold_in(own, 1), rows)]
    rotation = jax.random.randint(jax.random.fold_in(own, 2), (rows, 1), 0, top)
    return jnp.take_along_axis(table, (jnp.arange(top)[None, :] + rotation) % top, axis=1)


def shares(amount, total, reach, lean, full):
    weights = [(1 << 20) // math.isqrt(grade ** lean) + 1 for grade in range(1, amount + 1)]
    largest = reach if full else min(reach, max(-(-total // amount), total * weights[0] // sum(weights)))
    least = 1 if total - largest >= amount - 1 else 0
    counts, rest = [largest] + [least] * (amount - 1), total - largest - least * (amount - 1)
    while rest > 0:
        candidates = [i for i in range(1, amount) if counts[i] < largest] or [i for i in range(1, amount) if counts[i] < reach]
        whole, left = sum([weights[i] for i in candidates]), rest
        for i in candidates:
            extra = min(reach - counts[i], max(1, left * weights[i] // whole), rest)
            counts[i] = counts[i] + extra
            rest = rest - extra
    return np.array(counts)


def gaussian(own_key, shape, deviation, most, pieces=(), kind=jnp.bfloat16):
    drawn = jax.random.normal(own_key, shape, jnp.float32) * deviation
    if len(pieces) > 0:
        drawn = levels(own_key, shape, pieces, -0.22, 0.18) * drawn
    return jnp.clip(drawn, min=-most, max=most).astype(kind)


def setup_inputs(seed: int = 0) -> dict:
    seeds = jax.random.split(jax.random.key(seed), 8)
    velocity = gaussian(seeds[0], (3, ELEMS, NODES), 1.0, 6.0, ((1, 128),), jnp.float32)
    positions = gaussian(seeds[1], (3, ROWS, COLS), 1.0, 6.0, ((1, 128),), jnp.float32)
    stiff_h = jnp.clip(jnp.exp(math.log(1.0) - 2.3025851 * jax.random.uniform(seeds[2], (ROWS, COLS), jnp.float32) ** levels(seeds[2], (ROWS, COLS), ((0, 128),), -0.2, 0.2)), 0.1, 1.0)
    stiff_v = jnp.clip(jnp.exp(math.log(1.0) - 2.3025851 * jax.random.uniform(seeds[3], (ROWS, COLS), jnp.float32) ** levels(seeds[3], (ROWS, COLS), ((0, 128),), -0.2, 0.2)), 0.1, 1.0)
    marker_owner_keys = jax.random.split(jax.random.fold_in(seeds[4], 1), MARKERS // M_DEV)
    marker_owner_turns = jax.random.permutation(jax.random.fold_in(seeds[4], 3), MARKERS // M_DEV)
    marker_owner = jax.vmap(lambda own, number: assign_block(jax.random.fold_in(seeds[4], 2), own, number, M_DEV, DEVICES, 1, CAP, 2))(marker_owner_keys, marker_owner_turns).reshape((MARKERS, 1))
    marker_element = plant(jax.random.randint(seeds[5], (MARKERS,), 0, E_DEV), jax.random.fold_in(seeds[5], 1), 0, E_DEV - 1).astype(jnp.int32)
    marker_coords = jnp.clip(jax.random.uniform(seeds[6], (3, MARKERS), jnp.float32, -1.0, 1.0) * levels(seeds[6], (3, MARKERS), ((1, 128),), -0.4, 0.0), -1.0, 1.0)
    return {"velocity": velocity, "positions": positions, "stiff_h": stiff_h, "stiff_v": stiff_v, "marker_owner": marker_owner, "marker_element": marker_element, "marker_coords": marker_coords}


bend_modulus = 0.05
time_step = 0.5


def basis(values):
    abscissa = -jnp.cos(jnp.pi * jnp.arange(POINTS).astype(values.dtype) / (POINTS - 1))
    collected = []
    for i in range(POINTS):
        product = jnp.ones_like(values)
        for j in range(POINTS):
            if j != i:
                product = product * ((values - abscissa[j]) / (abscissa[i] - abscissa[j]))
        collected.append(product)
    return jnp.stack(collected)


def weight_table(factors):
    along_r = factors[0:POINTS].T
    along_s = factors[POINTS:2 * POINTS].T
    along_t = factors[2 * POINTS:3 * POINTS].T
    table = along_r[:, :, None, None] * along_s[:, None, :, None] * along_t[:, None, None, :]
    return table.reshape(along_r.shape[0], POINTS * POINTS * POINTS)


def surface_laplacian(extended):
    middle = extended[:, 1:-1]
    return extended[:, 2:] + extended[:, :-2] + jnp.roll(middle, 1, axis=2) + jnp.roll(middle, -1, axis=2) - 4.0 * middle


def tension(extended, stiff_h):
    points = extended[:3]
    vertical = extended[3]
    middle = points[:, 1:-1]
    return (stiff_h * (jnp.roll(middle, -1, axis=2) - middle)
            + jnp.roll(stiff_h, 1, axis=1) * (jnp.roll(middle, 1, axis=2) - middle)
            + vertical[1:-1] * (points[:, 2:] - middle)
            + vertical[:-2] * (points[:, :-2] - middle))


def wrap_rows(array):
    return jnp.concatenate([array[:, -1:], array, array[:, :1]], axis=1)


def reference(velocity, positions, stiff_h, stiff_v, marker_owner, marker_element, marker_coords):
    stacked = jnp.concatenate([positions, stiff_v[None]], axis=0)
    extended = wrap_rows(stacked)
    pulling = tension(extended, stiff_h)
    laplace = surface_laplacian(extended[:3])
    bending = -bend_modulus * surface_laplacian(wrap_rows(laplace))
    marker_force = (pulling + bending).reshape(3, MARKERS)
    element_ids = (marker_owner[:, 0] * E_DEV + marker_element).astype(jnp.int32)
    factors = jnp.concatenate([basis(marker_coords[0]), basis(marker_coords[1]), basis(marker_coords[2])], axis=0)
    factor_blocks = factors.reshape(3 * POINTS, DEVICES, M_DEV).transpose(1, 0, 2)
    element_blocks = element_ids.reshape(DEVICES, M_DEV)
    force_blocks = marker_force.reshape(3, DEVICES, M_DEV).transpose(1, 0, 2)

    def advance(running, inputs):
        block_factors, block_elements, pushes = inputs
        weights = weight_table(block_factors)
        gathered = jnp.take(velocity, block_elements, axis=1)
        sampled = jnp.sum(gathered * weights[None], axis=-1)
        running = running.at[:, block_elements, :].add(pushes[:, :, None] * weights[None])
        return running, sampled

    node_forces, sampled = lax.scan(advance, jnp.zeros_like(velocity), (factor_blocks, element_blocks, force_blocks))
    moved = sampled.transpose(1, 0, 2).reshape(3, ROWS, COLS)
    return positions + time_step * moved, node_forces
```

```python
import math

import jax
import jax.numpy as jnp
import numpy as np
from jax import lax
from jax.experimental import pallas as pl
from jax.experimental.pallas import tpu as pltpu
from jax.sharding import PartitionSpec as P

POINTS = 8
NODES = 512
ELEMS = 256
ROWS = 32
COLS = 256
DEVICES = 128
LANES = 128
HALF = 64
TILES = 96
CHUNK = 512
CHUNK_TILES = CHUNK // LANES
COMP_TILES = 100

bend_modulus = 0.05
time_step = 0.5

BF = jnp.bfloat16
F32 = jnp.float32
I32 = jnp.int32
NN = (((1,), (0,)), ((), ()))
NT = (((1,), (1,)), ((), ()))


def dot(a, b, dims=NN):
    return lax.dot_general(a, b, dims, preferred_element_type=F32)


def iota(shape, dim):
    return lax.broadcasted_iota(I32, shape, dim)


def one_hot(row, count):
    hit = jnp.broadcast_to(row, (count, row.shape[1])) == iota((count, row.shape[1]), 0)
    return jnp.where(hit, 1.0, 0.0).astype(BF)


def split(x):
    high = x.astype(BF)
    return high, (x - high.astype(F32)).astype(BF)


def basis_tables():
    nodes = -np.cos(np.pi * np.arange(POINTS, dtype=np.float64) / (POINTS - 1))
    nodes = nodes.astype(np.float32).astype(np.float64)
    scale = np.zeros((POINTS, POINTS))
    for j in range(POINTS):
        for i in range(POINTS):
            if i != j:
                scale[j, i] = 1.0 / (nodes[i] - nodes[j])
    scale = np.broadcast_to(scale[:, :, None], (POINTS, POINTS, LANES))
    return nodes, np.ascontiguousarray(scale, np.float32)


NODE_AT, SCALE_OF = basis_tables()


def basis(row, scale):
    n = row.shape[1]
    x = jnp.broadcast_to(row, (POINTS, n))
    which = iota((POINTS, n), 0)
    product = None
    for j in range(POINTS):
        s = jnp.concatenate([scale[j]] * (n // LANES), axis=1)
        factor = jnp.where(which == j, 1.0, (x - float(NODE_AT[j])) * s)
        product = factor if product is None else product * factor
    return product


def dispatch(below, above, positions, stiff_h, stiff_v, owner, element, coords,
             send, slot, ext, vals, pre, cnt, acc):
    ext[:, 8:8 + ROWS] = jnp.concatenate([positions[...], stiff_v[...][None]], axis=0)
    ext[:, 6:8] = below[...]
    ext[:, 8 + ROWS:10 + ROWS] = above[...]

    def rows(k, first, count):
        return ext[k, first + 8:first + 8 + count]

    sh = stiff_h[...]
    sh_left = pltpu.roll(sh, 1, 1)
    sv = rows(3, 0, ROWS)
    sv_below = rows(3, -1, ROWS)
    for k in range(3):
        mid = rows(k, 0, ROWS)
        pull = (
            sh * (pltpu.roll(mid, COLS - 1, 1) - mid)
            + sh_left * (pltpu.roll(mid, 1, 1) - mid)
            + sv * (rows(k, 1, ROWS) - mid)
            + sv_below * (rows(k, -1, ROWS) - mid)
        )

        def lap_at(first):
            m = rows(k, first, ROWS)
            return (
                rows(k, first + 1, ROWS)
                + rows(k, first - 1, ROWS)
                + pltpu.roll(m, 1, 1)
                + pltpu.roll(m, COLS - 1, 1)
                - 4.0 * m
            )

        lap = lap_at(0)
        bend = (
            lap_at(1)
            + lap_at(-1)
            + pltpu.roll(lap, 1, 1)
            + pltpu.roll(lap, COLS - 1, 1)
            - 4.0 * lap
        )
        force = pull - bend_modulus * bend
        c = coords[k]
        for i, v in ((k, c), (3 + k, force)):
            high = v.astype(BF).astype(F32)
            vals[2 * i] = high
            vals[2 * i + 1] = v - high
    vals[12] = element[...].astype(F32)

    before = jnp.where(iota((COLS, COLS), 0) < iota((COLS, COLS), 1), 1.0, 0.0).astype(BF)
    table = jnp.concatenate([before, jnp.ones((COLS, LANES), BF)], axis=1)

    @pl.loop(0, ROWS, unroll=4)
    def _(r):
        hot = one_hot(owner[pl.ds(r, 1), :], DEVICES)
        p = dot(hot, table)
        pre[r] = p[:, :COLS]
        cnt[r] = p[:, COLS:]

    def rank_rows(r, base):
        own = owner[pl.ds(r, 1), :]
        hit = jnp.broadcast_to(own, (DEVICES, COLS)) == iota((DEVICES, COLS), 0)
        both = jnp.concatenate([base, base], axis=1)
        rank = jnp.sum(jnp.where(hit, pre[r] + both, 0.0), axis=0, keepdims=True)
        slot[pl.ds(r, 1), :] = own * LANES + rank.astype(I32)
        return base + cnt[r]

    total = lax.fori_loop(0, ROWS, rank_rows, jnp.zeros((DEVICES, LANES), F32), unroll=4)

    acc[...] = jnp.zeros_like(acc)

    @pl.loop(0, ROWS, unroll=2)
    def _(r):
        p = slot[pl.ds(r, 1), :]
        low = one_hot(jnp.bitwise_and(p, 255), 256)
        hit = jnp.broadcast_to(lax.shift_right_logical(p, 8), (HALF, COLS)) == iota((HALF, COLS), 0)

        def picked(i):
            row = jnp.broadcast_to(vals[i, pl.ds(r, 1), :], (HALF, COLS))
            return jnp.where(hit, row, 0.0).astype(BF)

        highs = jnp.concatenate([picked(2 * i) for i in range(7)], axis=0)
        lows = jnp.concatenate([picked(2 * i + 1) for i in range(6)], axis=0)
        acc[:6 * HALF] += dot(highs[:6 * HALF], low, NT) + dot(lows, low, NT)
        acc[6 * HALF:] += dot(highs[6 * HALF:], low, NT)

    for i in range(7):
        v = acc[i * HALF:(i + 1) * HALF]
        send[:, i, :] = v[:, :LANES]
        send[:, 8 + i, :] = v[:, LANES:]
    cnt[0] = total
    send[:, 7, :] = cnt[0, pl.ds(0, HALF, stride=2), :]
    send[:, 15, :] = cnt[0, pl.ds(1, HALF, stride=2), :]


def run_dispatch(below, above, positions, stiff_h, stiff_v, owner, element, coords):
    return pl.pallas_call(
        dispatch,
        out_shape=(
            jax.ShapeDtypeStruct((HALF, 16, LANES), F32),
            jax.ShapeDtypeStruct((ROWS, COLS), I32),
        ),
        in_specs=[pl.BlockSpec(memory_space=pltpu.VMEM)] * 8,
        out_specs=(pl.BlockSpec(memory_space=pltpu.VMEM),) * 2,
        scratch_shapes=[
            pltpu.VMEM((4, ROWS + 16, COLS), F32),
            pltpu.VMEM((13, ROWS, COLS), F32),
            pltpu.VMEM((ROWS, DEVICES, COLS), F32),
            pltpu.VMEM((ROWS, DEVICES, LANES), F32),
            pltpu.VMEM((7 * HALF, COLS), F32),
        ],
        name="dispatch",
    )(below, above, positions, stiff_h, stiff_v, owner, element, coords)


def tile_rows(comp, first, value):
    return jnp.concatenate([comp[first + t, value:value + 1, :] for t in range(CHUNK_TILES)], axis=1)


def sample(recv, velocity, scale, back, comp, total, vt, sampled, offs_v, offs, sem):
    counts = recv[:, 7, :]
    by_lane = jnp.transpose(counts)[:8].astype(BF)
    upto = jnp.where(iota((LANES, LANES), 0) < iota((LANES, LANES), 1), 1.0, 0.0).astype(BF)
    whole = jnp.ones((LANES, LANES), BF)
    offs_v[...] = jnp.concatenate([dot(by_lane, upto), dot(by_lane, whole)], axis=0).astype(I32)
    copy = pltpu.make_async_copy(offs_v, offs, sem)
    copy.start()
    for k in range(3):
        high, low = split(jnp.transpose(velocity[k]))
        vt[k * NODES:(k + 1) * NODES, :ELEMS] = high
        vt[k * NODES:(k + 1) * NODES, ELEMS:] = low
    copy.wait()
    comp[0] = jnp.zeros((8, LANES), F32)
    lane = iota((8, LANES), 1)

    @pl.loop(0, DEVICES, unroll=8)
    def _(s):
        off = offs[0, s]
        turn = jnp.bitwise_and(off, LANES - 1)
        first = lax.shift_right_logical(off, 7)
        turned = pltpu.roll(recv[s], turn, 1)
        comp[first] = comp[first] + jnp.where(lane >= turn, turned, 0.0)
        comp[first + 1] = jnp.where(lane < turn, turned, 0.0)

    count = offs[8, 0]
    total[0] = count
    used = lax.shift_right_logical(count + (LANES - 1), 7)
    for t in range(CHUNK_TILES):
        comp[used + t] = jnp.zeros((8, LANES), F32)
    steps = lax.shift_right_logical(count + (CHUNK - 1), int(math.log2(CHUNK)))
    table = scale[...]

    @pl.loop(0, steps)
    def _(j):
        first = j * CHUNK_TILES
        hot = one_hot(tile_rows(comp, first, 6).astype(I32), ELEMS)
        hot2 = jnp.concatenate([hot, hot], axis=0)
        along_r = basis(tile_rows(comp, first, 0), table)
        along_s = basis(tile_rows(comp, first, 1), table)
        along_t = basis(tile_rows(comp, first, 2), table)
        out = []
        for k in range(3):
            gk = dot(vt[k * NODES:(k + 1) * NODES, :], hot2)
            over_r = None
            for a in range(POINTS):
                term = gk[a * 64:(a + 1) * 64] * along_r[a:a + 1]
                over_r = term if over_r is None else over_r + term
            over_s = None
            for b in range(POINTS):
                term = over_r[b * 8:(b + 1) * 8] * along_s[b:b + 1]
                over_s = term if over_s is None else over_s + term
            out.append(jnp.sum(over_s * along_t, axis=0, keepdims=True))
        for t in range(CHUNK_TILES):
            for k in range(3):
                sampled[first + t, k:k + 1, :] = out[k][:, t * LANES:(t + 1) * LANES]

    sampled[used] = jnp.zeros((4, LANES), F32)
    sampled[used + 1] = jnp.zeros((4, LANES), F32)
    lane4 = iota((4, LANES), 1)

    @pl.loop(0, DEVICES, unroll=8)
    def _(s):
        off = offs[0, s]
        turn = jnp.bitwise_and(off, LANES - 1)
        first = lax.shift_right_logical(off, 7)
        both = jnp.where(lane4 >= turn, sampled[first], sampled[first + 1])
        back[s] = pltpu.roll(both, jnp.bitwise_and(LANES - turn, LANES - 1), 1)


def run_sample(recv, velocity):
    return pl.pallas_call(
        sample,
        out_shape=(
            jax.ShapeDtypeStruct((DEVICES, 4, LANES), F32),
            jax.ShapeDtypeStruct((COMP_TILES, 8, LANES), F32),
            jax.ShapeDtypeStruct((1,), I32),
        ),
        in_specs=[pl.BlockSpec(memory_space=pltpu.VMEM)] * 3,
        out_specs=(
            pl.BlockSpec(memory_space=pltpu.VMEM),
            pl.BlockSpec(memory_space=pltpu.VMEM),
            pl.BlockSpec(memory_space=pltpu.SMEM),
        ),
        scratch_shapes=[
            pltpu.VMEM((3 * NODES, 2 * ELEMS), BF),
            pltpu.VMEM((COMP_TILES, 4, LANES), F32),
            pltpu.VMEM((16, LANES), I32),
            pltpu.SMEM((16, LANES), I32),
            pltpu.SemaphoreType.DMA,
        ],
        name="sample",
    )(recv, velocity, jnp.asarray(SCALE_OF))


def deposit(total, comp, scale, out, acc, loads):
    acc[...] = jnp.zeros_like(acc)
    steps = lax.shift_right_logical(total[0] + (CHUNK - 1), int(math.log2(CHUNK)))
    table = scale[...]

    @pl.loop(0, steps)
    def _(j):
        first = j * CHUNK_TILES
        hot = one_hot(tile_rows(comp, first, 6).astype(I32), ELEMS)
        hot2 = jnp.concatenate([hot, hot], axis=1)
        along_r = basis(tile_rows(comp, first, 0), table)
        along_s = basis(tile_rows(comp, first, 1), table)
        along_t = basis(tile_rows(comp, first, 2), table)
        plane = jnp.concatenate([along_s[b:b + 1] * along_t for b in range(POINTS)], axis=0)
        for k in range(3):
            push = along_r * tile_rows(comp, first, 3 + k)
            for a in range(POINTS):
                high, low = split(plane * push[a:a + 1])
                at = k * NODES + a * 64
                loads[at:at + 64, :CHUNK] = high
                loads[at:at + 64, CHUNK:] = low
            at = k * NODES
            acc[at:at + NODES] += dot(loads[at:at + NODES], hot2, NT)

    for k in range(3):
        out[k] = jnp.transpose(acc[k * NODES:(k + 1) * NODES])


def run_deposit(total, comp):
    return pl.pallas_call(
        deposit,
        out_shape=jax.ShapeDtypeStruct((3, ELEMS, NODES), F32),
        in_specs=[
            pl.BlockSpec(memory_space=pltpu.SMEM),
            pl.BlockSpec(memory_space=pltpu.VMEM),
            pl.BlockSpec(memory_space=pltpu.VMEM),
        ],
        out_specs=pl.BlockSpec(memory_space=pltpu.VMEM),
        scratch_shapes=[pltpu.VMEM((3 * NODES, ELEMS), F32), pltpu.VMEM((3 * NODES, 2 * CHUNK), BF)],
        name="deposit",
    )(total, comp, jnp.asarray(SCALE_OF))


def collect(got, slot, positions, out, table):
    for k in range(3):
        both = jnp.concatenate([got[:, k, :], got[:, 4 + k, :]], axis=1)
        high, low = split(both)
        table[k * HALF:(k + 1) * HALF, :COLS] = high
        table[k * HALF:(k + 1) * HALF, COLS:] = low

    @pl.loop(0, ROWS, unroll=4)
    def _(r):
        p = slot[pl.ds(r, 1), :]
        low = one_hot(jnp.bitwise_and(p, 255), 256)
        hit = jnp.broadcast_to(lax.shift_right_logical(p, 8), (HALF, COLS)) == iota((HALF, COLS), 0)
        g = dot(table[...], jnp.concatenate([low, low], axis=0))
        for k in range(3):
            mine = jnp.sum(jnp.where(hit, g[k * HALF:(k + 1) * HALF], 0.0), axis=0, keepdims=True)
            out[k, pl.ds(r, 1), :] = positions[k, pl.ds(r, 1), :] + time_step * mine


def run_collect(got, slot, positions):
    return pl.pallas_call(
        collect,
        out_shape=jax.ShapeDtypeStruct((3, ROWS, COLS), F32),
        in_specs=[pl.BlockSpec(memory_space=pltpu.VMEM)] * 3,
        out_specs=pl.BlockSpec(memory_space=pltpu.VMEM),
        scratch_shapes=[pltpu.VMEM((3 * HALF, 2 * COLS), BF)],
        name="collect",
    )(got, slot, positions)


def edges(positions, stiff_v):
    stacked = jnp.concatenate([positions, stiff_v[None]], axis=0)
    axes = ("gx", "gy")
    peers = lax.axis_size("gx") * lax.axis_size("gy")
    up = [(i, (i + 1) % peers) for i in range(peers)]
    below = lax.ppermute(stacked[:, ROWS - 2:], axes, up)
    above = lax.ppermute(stacked[:, :2], axes, [(b, a) for a, b in up])
    return below, above


def local(velocity, positions, stiff_h, stiff_v, marker_owner, marker_element, marker_coords):
    owner = marker_owner.reshape(ROWS, COLS)
    element = marker_element.reshape(ROWS, COLS)
    coords = marker_coords.reshape(3, ROWS, COLS)
    below, above = edges(positions, stiff_v)
    send, slot = run_dispatch(below, above, positions, stiff_h, stiff_v, owner, element, coords)
    recv = lax.all_to_all(
        send.reshape(DEVICES, 8, LANES), ("gx", "gy"), split_axis=0, concat_axis=0, tiled=True
    )
    back, comp, total = run_sample(recv, velocity)
    got = lax.all_to_all(back, ("gx", "gy"), split_axis=0, concat_axis=0, tiled=True)
    node_forces = run_deposit(total, comp)
    moved = run_collect(got.reshape(HALF, 8, LANES), slot, positions)
    return moved, node_forces


def solution(mesh):
    return jax.shard_map(
        local,
        mesh=mesh,
        in_specs=(
            P(None, ("gx", "gy"), None),
            P(None, ("gx", "gy"), None),
            P(("gx", "gy"), None),
            P(("gx", "gy"), None),
            P(("gx", "gy"), None),
            P(("gx", "gy")),
            P(None, ("gx", "gy")),
        ),
        out_specs=(P(None, ("gx", "gy"), None), P(None, ("gx", "gy"), None)),
        check_vma=False,
    )
```

```python
import math

import jax
import jax.numpy as jnp
import numpy as np
from jax import lax
from jax.experimental import pallas as pl
from jax.experimental.pallas import tpu as pltpu
from jax.sharding import PartitionSpec as P

POINTS = 8
NODES = 512
ELEMS = 256
ROWS = 32
COLS = 256
DEVICES = 128
LANES = 128
HALF = 64
TILES = 96
CHUNK = 512
CHUNK_TILES = CHUNK // LANES
CAP = 96
GROUPS = 8
PER_GROUP = DEVICES // GROUPS

bend_modulus = 0.05
time_step = 0.5

BF = jnp.bfloat16
F32 = jnp.float32
I32 = jnp.int32
NN = (((1,), (0,)), ((), ()))
NT = (((1,), (1,)), ((), ()))


def dot(a, b, dims=NN):
    return lax.dot_general(a, b, dims, preferred_element_type=F32)


def iota(shape, dim):
    return lax.broadcasted_iota(I32, shape, dim)


def one_hot(row, count):
    hit = jnp.broadcast_to(row, (count, row.shape[1])) == iota((count, row.shape[1]), 0)
    return jnp.where(hit, 1.0, 0.0).astype(BF)


def split(x):
    high = x.astype(BF)
    return high, (x - high.astype(F32)).astype(BF)


def basis_tables():
    nodes = -np.cos(np.pi * np.arange(POINTS, dtype=np.float64) / (POINTS - 1))
    nodes = nodes.astype(np.float32).astype(np.float64)
    scale = np.zeros((POINTS, POINTS))
    for j in range(POINTS):
        for i in range(POINTS):
            if i != j:
                scale[j, i] = 1.0 / (nodes[i] - nodes[j])
    scale = np.broadcast_to(scale[:, :, None], (POINTS, POINTS, LANES))
    return nodes, np.ascontiguousarray(scale, np.float32)


NODE_AT, SCALE_OF = basis_tables()


def basis(row, scale):
    n = row.shape[1]
    x = jnp.broadcast_to(row, (POINTS, n))
    which = iota((POINTS, n), 0)
    product = None
    for j in range(POINTS):
        s = jnp.concatenate([scale[j]] * (n // LANES), axis=1)
        factor = jnp.where(which == j, 1.0, (x - float(NODE_AT[j])) * s)
        product = factor if product is None else product * factor
    return product

MESH = pl.DeviceIdType.MESH


def place(index):
    return (index // 4, index % 4)


def tile_rows(comp, first, value):
    return jnp.concatenate([comp[first + t, value:value + 1, :] for t in range(CHUNK_TILES)], axis=1)


def forces(ext, stiff_h, vals):
    def rows(k, first, count):
        return ext[k, first + 8:first + 8 + count]

    sh = stiff_h[...]
    sh_left = pltpu.roll(sh, 1, 1)
    sv = rows(3, 0, ROWS)
    sv_below = rows(3, -1, ROWS)
    for k in range(3):
        mid = rows(k, 0, ROWS)
        pull = (
            sh * (pltpu.roll(mid, COLS - 1, 1) - mid)
            + sh_left * (pltpu.roll(mid, 1, 1) - mid)
            + sv * (rows(k, 1, ROWS) - mid)
            + sv_below * (rows(k, -1, ROWS) - mid)
        )

        def lap_at(first):
            m = rows(k, first, ROWS)
            return (
                rows(k, first + 1, ROWS)
                + rows(k, first - 1, ROWS)
                + pltpu.roll(m, 1, 1)
                + pltpu.roll(m, COLS - 1, 1)
                - 4.0 * m
            )

        lap = lap_at(0)
        bend = (
            lap_at(1)
            + lap_at(-1)
            + pltpu.roll(lap, 1, 1)
            + pltpu.roll(lap, COLS - 1, 1)
            - 4.0 * lap
        )
        force = pull - bend_modulus * bend
        high = force.astype(BF).astype(F32)
        vals[2 * k] = high
        vals[2 * k + 1] = force - high


def step(positions, stiff_h, stiff_v, owner, element, coords, velocity, scale,
         moved, out,
         ext, halo, vals, slot, acc, send, recv, comp, sampled, back, got, table,
         vel, vt, force_acc, loads,
         vel_sem, halo_send, halo_recv, send_sem, recv_sem, back_send, back_recv):
    me = lax.axis_index("gx") * 4 + lax.axis_index("gy")
    up, down = lax.rem(me + 1, DEVICES), lax.rem(me + DEVICES - 1, DEVICES)
    barrier = pltpu.get_barrier_semaphore()

    @pl.loop(1, DEVICES)
    def _(j):
        pl.semaphore_signal(
            barrier, inc=1, device_id=place(lax.rem(me + j, DEVICES)), device_id_type=MESH
        )

    fetch = pltpu.make_async_copy(velocity, vel, vel_sem)
    fetch.start()

    before = jnp.where(iota((COLS, COLS), 0) < iota((COLS, COLS), 1), 1.0, 0.0).astype(BF)
    counting = jnp.concatenate([before, jnp.ones((COLS, LANES), BF)], axis=1)

    def rank_rows(r, base):
        own = owner[:, pl.ds(pl.multiple_of(r * COLS, COLS), COLS)]
        hit = jnp.broadcast_to(own, (DEVICES, COLS)) == iota((DEVICES, COLS), 0)
        p = dot(jnp.where(hit, 1.0, 0.0).astype(BF), counting)
        both = jnp.concatenate([base, base], axis=1)
        rank = jnp.sum(jnp.where(hit, p[:, :COLS] + both, 0.0), axis=0, keepdims=True)
        slot[pl.ds(r, 1), :] = own * LANES + rank.astype(I32)
        return base + p[:, COLS:]

    lax.fori_loop(0, ROWS, rank_rows, jnp.zeros((DEVICES, LANES), F32), unroll=4)

    pl.semaphore_wait(barrier, DEVICES - 1)

    last, lead = pl.ds(ROWS - 8, 8), pl.ds(0, 8)
    edge_copies = []
    for i, (target, side, part) in enumerate(((up, 0, last), (down, 1, lead))):
        for src, dst, n in (
            (positions.at[:, part, :], halo.at[side, pl.ds(0, 3)], 2 * i),
            (stiff_v.at[part, :], halo.at[side, 3], 2 * i + 1),
        ):
            edge_copies.append(
                pltpu.make_async_remote_copy(
                    src_ref=src,
                    dst_ref=dst,
                    send_sem=halo_send.at[n],
                    recv_sem=halo_recv.at[n],
                    device_id=place(target),
                    device_id_type=MESH,
                )
            )
    for copy in edge_copies:
        copy.start()
    fetch.wait()
    for k in range(3):
        high, low = split(jnp.transpose(vel[k]))
        vt[k * NODES:(k + 1) * NODES, :ELEMS] = high
        vt[k * NODES:(k + 1) * NODES, ELEMS:] = low
    ext[:, 8:8 + ROWS] = jnp.concatenate([positions[...], stiff_v[...][None]], axis=0)
    for copy in edge_copies:
        copy.wait()
    ext[:, 6:8] = halo[0, :, 6:8, :]
    ext[:, 8 + ROWS:10 + ROWS] = halo[1, :, 0:2, :]
    forces(ext, stiff_h, vals)

    acc[...] = jnp.zeros_like(acc)

    @pl.loop(0, ROWS, unroll=2)
    def _(r):
        at = pl.ds(pl.multiple_of(r * COLS, COLS), COLS)
        p = slot[pl.ds(r, 1), :]
        low_hot = one_hot(jnp.bitwise_and(p, 255), 256)
        hit = jnp.broadcast_to(lax.shift_right_logical(p, 8), (HALF, COLS)) == iota((HALF, COLS), 0)

        def picked(row):
            return jnp.where(hit, jnp.broadcast_to(row, (HALF, COLS)), 0.0).astype(BF)

        highs, lows = [], []
        for k in range(3):
            row = coords[k:k + 1, at]
            high = row.astype(BF).astype(F32)
            highs.append(picked(high))
            lows.append(picked(row - high))
        for k in range(3):
            highs.append(picked(vals[2 * k, pl.ds(r, 1), :]))
            lows.append(picked(vals[2 * k + 1, pl.ds(r, 1), :]))
        whole = picked(element[:, at].astype(F32))
        highs = jnp.concatenate(highs, axis=0)
        lows = jnp.concatenate(lows, axis=0)
        acc[:6 * HALF] += dot(highs, low_hot, NT) + dot(lows, low_hot, NT)
        acc[6 * HALF:] += dot(whole, low_hot, NT)

    for i in range(7):
        v = acc[i * HALF:(i + 1) * HALF]
        send[:, i, :] = v[:, :LANES]
        send[:, 8 + i, :] = v[:, LANES:]
    send[:, 7, :] = jnp.zeros((HALF, LANES), F32)
    send[:, 15, :] = jnp.zeros((HALF, LANES), F32)

    def block_of(t):
        return send.at[t // 2, pl.ds(pl.multiple_of(lax.rem(t, 2) * 8, 8), 8), :]

    def outward(j):
        t = lax.rem(me + j, DEVICES)
        return pltpu.make_async_remote_copy(
            src_ref=block_of(t),
            dst_ref=recv.at[me],
            send_sem=send_sem.at[j],
            recv_sem=recv_sem.at[j],
            device_id=place(t),
            device_id_type=MESH,
        )

    def homeward(j):
        t = lax.rem(me + DEVICES - j, DEVICES)
        return pltpu.make_async_remote_copy(
            src_ref=back.at[t],
            dst_ref=got.at[me],
            send_sem=back_send.at[j],
            recv_sem=back_recv.at[j],
            device_id=place(t),
            device_id_type=MESH,
        )

    @pl.loop(1, DEVICES)
    def _(j):
        outward(j).start()

    recv[me] = send[me // 2, pl.ds(pl.multiple_of(lax.rem(me, 2) * 8, 8), 8), :]
    force_acc[...] = jnp.zeros_like(force_acc)
    sampled[...] = jnp.zeros_like(sampled)
    scales = scale[...]
    lane8 = iota((8, LANES), 1)
    lane4 = iota((4, LANES), 1)

    def source(j):
        return lax.rem(me + DEVICES - j, DEVICES)

    @pl.loop(0, GROUPS)
    def _(g):
        @pl.loop(0, PER_GROUP)
        def _(i):
            @pl.when(g * PER_GROUP + i > 0)
            def _():
                outward(g * PER_GROUP + i).wait_recv()

        @pl.loop(0, PER_GROUP // 4)
        def _(q):
            b = [recv[source(g * PER_GROUP + q * 4 + i)] for i in range(4)]
            r1 = pltpu.roll(b[1], 96, 1)
            r2 = pltpu.roll(b[2], 64, 1)
            r3 = pltpu.roll(b[3], 32, 1)
            comp[q * 3] = jnp.where(lane8 < 96, b[0], r1)
            comp[q * 3 + 1] = jnp.where(lane8 < 64, r1, r2)
            comp[q * 3 + 2] = jnp.where(lane8 < 32, r2, r3)

        @pl.loop(0, PER_GROUP * CAP // CHUNK)
        def _(c):
            first = c * CHUNK_TILES
            hot = one_hot(tile_rows(comp, first, 6).astype(I32), ELEMS)
            along_r = basis(tile_rows(comp, first, 0), scales)
            along_s = basis(tile_rows(comp, first, 1), scales)
            along_t = basis(tile_rows(comp, first, 2), scales)
            stacked = jnp.concatenate([hot, hot], axis=0)
            for k in range(3):
                gk = dot(vt[k * NODES:(k + 1) * NODES, :], stacked)
                over_r = None
                for a in range(POINTS):
                    term = gk[a * 64:(a + 1) * 64] * along_r[a:a + 1]
                    over_r = term if over_r is None else over_r + term
                over_s = None
                for b in range(POINTS):
                    term = over_r[b * 8:(b + 1) * 8] * along_s[b:b + 1]
                    over_s = term if over_s is None else over_s + term
                mine = jnp.sum(over_s * along_t, axis=0, keepdims=True)
                for t in range(CHUNK_TILES):
                    sampled[first + t, k:k + 1, :] = mine[:, t * LANES:(t + 1) * LANES]
            plane = jnp.concatenate([along_s[b:b + 1] * along_t for b in range(POINTS)], axis=0)
            beside = jnp.concatenate([hot, hot], axis=1)
            for k in range(3):
                push = along_r * tile_rows(comp, first, 3 + k)
                for a in range(POINTS):
                    high, low = split(plane * push[a:a + 1])
                    at = k * NODES + a * 64
                    loads[at:at + 64, :CHUNK] = high
                    loads[at:at + 64, CHUNK:] = low
                at = k * NODES
                force_acc[at:at + NODES] += dot(loads[at:at + NODES], beside, NT)

        @pl.loop(0, PER_GROUP // 4)
        def _(q):
            s = [sampled[q * 3 + i] for i in range(3)]
            j = g * PER_GROUP + q * 4
            back[source(j)] = s[0]
            back[source(j + 1)] = pltpu.roll(jnp.where(lane4 >= 96, s[0], s[1]), 32, 1)
            back[source(j + 2)] = pltpu.roll(jnp.where(lane4 >= 64, s[1], s[2]), 64, 1)
            back[source(j + 3)] = pltpu.roll(s[2], 96, 1)

        @pl.loop(0, PER_GROUP)
        def _(i):
            @pl.when(g * PER_GROUP + i > 0)
            def _():
                homeward(g * PER_GROUP + i).start()

    for k in range(3):
        out[k] = jnp.transpose(force_acc[k * NODES:(k + 1) * NODES])
    got[me] = back[me]

    @pl.loop(1, DEVICES)
    def _(j):
        homeward(j).wait_recv()

    for k in range(3):
        both = jnp.concatenate(
            [got[pl.ds(0, HALF, stride=2), k, :], got[pl.ds(1, HALF, stride=2), k, :]], axis=1
        )
        high, low = split(both)
        table[k * HALF:(k + 1) * HALF, :COLS] = high
        table[k * HALF:(k + 1) * HALF, COLS:] = low

    @pl.loop(0, ROWS, unroll=4)
    def _(r):
        p = slot[pl.ds(r, 1), :]
        low = one_hot(jnp.bitwise_and(p, 255), 256)
        hit = jnp.broadcast_to(lax.shift_right_logical(p, 8), (HALF, COLS)) == iota((HALF, COLS), 0)
        g = dot(table[...], jnp.concatenate([low, low], axis=0))
        for k in range(3):
            mine = jnp.sum(jnp.where(hit, g[k * HALF:(k + 1) * HALF], 0.0), axis=0, keepdims=True)
            moved[k, pl.ds(r, 1), :] = positions[k, pl.ds(r, 1), :] + time_step * mine

    @pl.loop(1, DEVICES)
    def _(j):
        outward(j).wait_send()
        homeward(j).wait_send()


def local(velocity, positions, stiff_h, stiff_v, marker_owner, marker_element, marker_coords):
    markers = ROWS * COLS
    group_tiles = PER_GROUP * CAP // LANES
    vmem = pl.BlockSpec(memory_space=pltpu.VMEM)
    return pl.pallas_call(
        step,
        out_shape=(
            jax.ShapeDtypeStruct((3, ROWS, COLS), F32),
            jax.ShapeDtypeStruct((3, ELEMS, NODES), F32),
        ),
        in_specs=[vmem] * 6 + [pl.BlockSpec(memory_space=pl.ANY), vmem],
        out_specs=(vmem, vmem),
        scratch_shapes=[
            pltpu.VMEM((4, ROWS + 16, COLS), F32),
            pltpu.VMEM((2, 4, 8, COLS), F32),
            pltpu.VMEM((6, ROWS, COLS), F32),
            pltpu.VMEM((ROWS, COLS), I32),
            pltpu.VMEM((7 * HALF, COLS), F32),
            pltpu.VMEM((HALF, 16, LANES), F32),
            pltpu.VMEM((DEVICES, 8, LANES), F32),
            pltpu.VMEM((group_tiles, 8, LANES), F32),
            pltpu.VMEM((group_tiles, 4, LANES), F32),
            pltpu.VMEM((DEVICES, 4, LANES), F32),
            pltpu.VMEM((DEVICES, 4, LANES), F32),
            pltpu.VMEM((3 * HALF, 2 * COLS), BF),
            pltpu.VMEM((3, ELEMS, NODES), F32),
            pltpu.VMEM((3 * NODES, 2 * ELEMS), BF),
            pltpu.VMEM((3 * NODES, ELEMS), F32),
            pltpu.VMEM((3 * NODES, 2 * CHUNK), BF),
            pltpu.SemaphoreType.DMA,
            pltpu.SemaphoreType.DMA((4,)),
            pltpu.SemaphoreType.DMA((4,)),
            pltpu.SemaphoreType.DMA((DEVICES,)),
            pltpu.SemaphoreType.DMA((DEVICES,)),
            pltpu.SemaphoreType.DMA((DEVICES,)),
            pltpu.SemaphoreType.DMA((DEVICES,)),
        ],
        compiler_params=pltpu.CompilerParams(collective_id=0, has_side_effects=True),
        name="step",
    )(
        positions, stiff_h, stiff_v,
        marker_owner.reshape(1, markers), marker_element.reshape(1, markers), marker_coords,
        velocity, jnp.asarray(SCALE_OF),
    )


def solution(mesh):
    return jax.shard_map(
        local,
        mesh=mesh,
        in_specs=(
            P(None, ("gx", "gy"), None),
            P(None, ("gx", "gy"), None),
            P(("gx", "gy"), None),
            P(("gx", "gy"), None),
            P(("gx", "gy"), None),
            P(("gx", "gy")),
            P(None, ("gx", "gy")),
        ),
        out_specs=(P(None, ("gx", "gy"), None), P(None, ("gx", "gy"), None)),
        check_vma=False,
    )
```

```python
import math

import jax
import jax.numpy as jnp
import numpy as np
from jax import lax
from jax.experimental import pallas as pl
from jax.experimental.pallas import tpu as pltpu
from jax.sharding import PartitionSpec as P

POINTS = 8
NODES = 512
ELEMS = 256
ROWS = 32
COLS = 256
DEVICES = 128
LANES = 128
HALF = 64
TILES = 96
CHUNK = 512
CHUNK_TILES = CHUNK // LANES
CAP = 96
GROUPS = 8
PER_GROUP = DEVICES // GROUPS

bend_modulus = 0.05
time_step = 0.5

BF = jnp.bfloat16
F32 = jnp.float32
I32 = jnp.int32
NN = (((1,), (0,)), ((), ()))
NT = (((1,), (1,)), ((), ()))


def dot(a, b, dims=NN):
    return lax.dot_general(a, b, dims, preferred_element_type=F32)


def iota(shape, dim):
    return lax.broadcasted_iota(I32, shape, dim)


def one_hot(row, count):
    hit = jnp.broadcast_to(row, (count, row.shape[1])) == iota((count, row.shape[1]), 0)
    return jnp.where(hit, 1.0, 0.0).astype(BF)


def split(x):
    high = x.astype(BF)
    return high, (x - high.astype(F32)).astype(BF)


def basis_tables():
    nodes = -np.cos(np.pi * np.arange(POINTS, dtype=np.float64) / (POINTS - 1))
    nodes = nodes.astype(np.float32).astype(np.float64)
    scale = np.zeros((POINTS, POINTS))
    for j in range(POINTS):
        for i in range(POINTS):
            if i != j:
                scale[j, i] = 1.0 / (nodes[i] - nodes[j])
    scale = np.broadcast_to(scale[:, :, None], (POINTS, POINTS, LANES))
    return nodes, np.ascontiguousarray(scale, np.float32)


NODE_AT, SCALE_OF = basis_tables()


def basis(row, scale):
    n = row.shape[1]
    x = jnp.broadcast_to(row, (POINTS, n))
    which = iota((POINTS, n), 0)
    product = None
    for j in range(POINTS):
        s = jnp.concatenate([scale[j]] * (n // LANES), axis=1)
        factor = jnp.where(which == j, 1.0, (x - float(NODE_AT[j])) * s)
        product = factor if product is None else product * factor
    return product

LOGICAL = pl.DeviceIdType.LOGICAL


def each_other(body):
    whole = (DEVICES - 1) // 8 * 8
    pl.loop(1, 1 + whole, unroll=8)(body)
    for j in range(1 + whole, DEVICES):
        body(j)


def tile_rows(comp, first, value):
    return jnp.concatenate([comp[first + t, value:value + 1, :] for t in range(CHUNK_TILES)], axis=1)


def forces(ext, stiff_h, vals):
    def rows(k, first, count):
        return ext[k, first + 8:first + 8 + count]

    sh = stiff_h[...]
    sh_left = pltpu.roll(sh, 1, 1)
    sv = rows(3, 0, ROWS)
    sv_below = rows(3, -1, ROWS)
    for k in range(3):
        mid = rows(k, 0, ROWS)
        pull = (
            sh * (pltpu.roll(mid, COLS - 1, 1) - mid)
            + sh_left * (pltpu.roll(mid, 1, 1) - mid)
            + sv * (rows(k, 1, ROWS) - mid)
            + sv_below * (rows(k, -1, ROWS) - mid)
        )

        def lap_at(first):
            m = rows(k, first, ROWS)
            return (
                rows(k, first + 1, ROWS)
                + rows(k, first - 1, ROWS)
                + pltpu.roll(m, 1, 1)
                + pltpu.roll(m, COLS - 1, 1)
                - 4.0 * m
            )

        lap = lap_at(0)
        bend = (
            lap_at(1)
            + lap_at(-1)
            + pltpu.roll(lap, 1, 1)
            + pltpu.roll(lap, COLS - 1, 1)
            - 4.0 * lap
        )
        force = pull - bend_modulus * bend
        high = force.astype(BF).astype(F32)
        vals[2 * k] = high
        vals[2 * k + 1] = force - high


def step(positions, stiff_h, stiff_v, owner, element, coords, velocity, scale,
         got_out, slot, force_acc,
         ext, halo, vals, acc, send, recv, comp, sampled, back, got,
         vel, vt, loads,
         vel_sem, halo_send, halo_recv, send_sem, recv_sem, back_send, back_recv):
    me = lax.axis_index("gx") * 4 + lax.axis_index("gy")
    up, down = lax.rem(me + 1, DEVICES), lax.rem(me + DEVICES - 1, DEVICES)
    barrier = pltpu.get_barrier_semaphore()

    @each_other
    def _(j):
        pl.semaphore_signal(
            barrier, inc=1, device_id=lax.rem(me + j, DEVICES), device_id_type=LOGICAL
        )

    fetch = pltpu.make_async_copy(velocity, vel, vel_sem)
    fetch.start()

    before = jnp.where(iota((COLS, COLS), 0) < iota((COLS, COLS), 1), 1.0, 0.0).astype(BF)
    counting = jnp.concatenate([before, jnp.ones((COLS, LANES), BF)], axis=1)

    def rank_rows(r, base):
        own = owner[:, pl.ds(pl.multiple_of(r * COLS, COLS), COLS)]
        hit = jnp.broadcast_to(own, (DEVICES, COLS)) == iota((DEVICES, COLS), 0)
        p = dot(jnp.where(hit, 1.0, 0.0).astype(BF), counting)
        both = jnp.concatenate([base, base], axis=1)
        rank = jnp.sum(jnp.where(hit, p[:, :COLS] + both, 0.0), axis=0, keepdims=True)
        slot[pl.ds(r, 1), :] = own * LANES + rank.astype(I32)
        return base + p[:, COLS:]

    lax.fori_loop(0, ROWS, rank_rows, jnp.zeros((DEVICES, LANES), F32), unroll=4)

    pl.semaphore_wait(barrier, DEVICES - 1)

    last, lead = pl.ds(ROWS - 8, 8), pl.ds(0, 8)
    edge_copies = []
    for i, (target, side, part) in enumerate(((up, 0, last), (down, 1, lead))):
        for src, dst, n in (
            (positions.at[:, part, :], halo.at[side, pl.ds(0, 3)], 2 * i),
            (stiff_v.at[part, :], halo.at[side, 3], 2 * i + 1),
        ):
            edge_copies.append(
                pltpu.make_async_remote_copy(
                    src_ref=src,
                    dst_ref=dst,
                    send_sem=halo_send.at[n],
                    recv_sem=halo_recv.at[n],
                    device_id=target,
                    device_id_type=LOGICAL,
                )
            )
    for copy in edge_copies:
        copy.start()
    fetch.wait()
    for k in range(3):
        high, low = split(jnp.transpose(vel[k]))
        vt[k * NODES:(k + 1) * NODES, :ELEMS] = high
        vt[k * NODES:(k + 1) * NODES, ELEMS:] = low
    ext[:, 8:8 + ROWS] = jnp.concatenate([positions[...], stiff_v[...][None]], axis=0)
    for copy in edge_copies:
        copy.wait()
    ext[:, 6:8] = halo[0, :, 6:8, :]
    ext[:, 8 + ROWS:10 + ROWS] = halo[1, :, 0:2, :]
    forces(ext, stiff_h, vals)

    acc[...] = jnp.zeros_like(acc)

    @pl.loop(0, ROWS, unroll=2)
    def _(r):
        at = pl.ds(pl.multiple_of(r * COLS, COLS), COLS)
        p = slot[pl.ds(r, 1), :]
        low_hot = one_hot(jnp.bitwise_and(p, 255), 256)
        hit = jnp.broadcast_to(lax.shift_right_logical(p, 8), (HALF, COLS)) == iota((HALF, COLS), 0)

        def picked(row):
            return jnp.where(hit, jnp.broadcast_to(row, (HALF, COLS)), 0.0).astype(BF)

        highs, lows = [], []
        for k in range(3):
            row = coords[k:k + 1, at]
            high = row.astype(BF).astype(F32)
            highs.append(picked(high))
            lows.append(picked(row - high))
        for k in range(3):
            highs.append(picked(vals[2 * k, pl.ds(r, 1), :]))
            lows.append(picked(vals[2 * k + 1, pl.ds(r, 1), :]))
        whole = picked(element[:, at].astype(F32))
        highs = jnp.concatenate(highs, axis=0)
        lows = jnp.concatenate(lows, axis=0)
        acc[:6 * HALF] += dot(highs, low_hot, NT) + dot(lows, low_hot, NT)
        acc[6 * HALF:] += dot(whole, low_hot, NT)

    for i in range(7):
        v = acc[i * HALF:(i + 1) * HALF]
        send[:, i, :] = v[:, :LANES]
        send[:, 8 + i, :] = v[:, LANES:]
    send[:, 7, :] = jnp.zeros((HALF, LANES), F32)
    send[:, 15, :] = jnp.zeros((HALF, LANES), F32)

    def block_of(t):
        return send.at[lax.div(t, 2), pl.ds(pl.multiple_of(lax.rem(t, 2) * 8, 8), 8), :]

    def outward(j):
        t = lax.rem(me + j, DEVICES)
        return pltpu.make_async_remote_copy(
            src_ref=block_of(t),
            dst_ref=recv.at[me],
            send_sem=send_sem,
            recv_sem=recv_sem.at[lax.div(j, PER_GROUP)],
            device_id=t,
            device_id_type=LOGICAL,
        )

    def homeward(j):
        t = lax.rem(me + DEVICES - j, DEVICES)
        return pltpu.make_async_remote_copy(
            src_ref=back.at[t],
            dst_ref=got.at[me],
            send_sem=back_send,
            recv_sem=back_recv,
            device_id=t,
            device_id_type=LOGICAL,
        )

    def arrived(ref, count, sem):
        part = ref.at[pl.ds(0, count)]
        pltpu.make_async_copy(part, part, sem).wait()

    @each_other
    def _(j):
        outward(j).start()

    recv[me] = send[me // 2, pl.ds(pl.multiple_of(lax.rem(me, 2) * 8, 8), 8), :]
    force_acc[...] = jnp.zeros_like(force_acc)
    sampled[...] = jnp.zeros_like(sampled)
    scales = scale[...]
    lane8 = iota((8, LANES), 1)
    lane4 = iota((4, LANES), 1)

    def source(j):
        return lax.rem(me + DEVICES - j, DEVICES)

    @pl.loop(0, GROUPS)
    def _(g):
        @pl.when(g == 0)
        def _():
            arrived(recv, PER_GROUP - 1, recv_sem.at[g])

        @pl.when(g > 0)
        def _():
            arrived(recv, PER_GROUP, recv_sem.at[g])

        for q in range(PER_GROUP // 4):
            b = [recv[source(g * PER_GROUP + q * 4 + i)] for i in range(4)]
            r1 = pltpu.roll(b[1], 96, 1)
            r2 = pltpu.roll(b[2], 64, 1)
            r3 = pltpu.roll(b[3], 32, 1)
            comp[q * 3] = jnp.where(lane8 < 96, b[0], r1)
            comp[q * 3 + 1] = jnp.where(lane8 < 64, r1, r2)
            comp[q * 3 + 2] = jnp.where(lane8 < 32, r2, r3)

        @pl.loop(0, PER_GROUP * CAP // CHUNK)
        def _(c):
            first = c * CHUNK_TILES
            hot = one_hot(tile_rows(comp, first, 6).astype(I32), ELEMS)
            along_r = basis(tile_rows(comp, first, 0), scales)
            along_s = basis(tile_rows(comp, first, 1), scales)
            along_t = basis(tile_rows(comp, first, 2), scales)
            stacked = jnp.concatenate([hot, hot], axis=0)
            for k in range(3):
                gk = dot(vt[k * NODES:(k + 1) * NODES, :], stacked)
                over_r = None
                for a in range(POINTS):
                    term = gk[a * 64:(a + 1) * 64] * along_r[a:a + 1]
                    over_r = term if over_r is None else over_r + term
                over_s = None
                for b in range(POINTS):
                    term = over_r[b * 8:(b + 1) * 8] * along_s[b:b + 1]
                    over_s = term if over_s is None else over_s + term
                mine = jnp.sum(over_s * along_t, axis=0, keepdims=True)
                for t in range(CHUNK_TILES):
                    sampled[first + t, k:k + 1, :] = mine[:, t * LANES:(t + 1) * LANES]
            plane = jnp.concatenate([along_s[b:b + 1] * along_t for b in range(POINTS)], axis=0)
            beside = jnp.concatenate([hot, hot], axis=1)
            for k in range(3):
                push = along_r * tile_rows(comp, first, 3 + k)
                for a in range(POINTS):
                    high, low = split(plane * push[a:a + 1])
                    at = k * NODES + a * 64
                    loads[at:at + 64, :CHUNK] = high
                    loads[at:at + 64, CHUNK:] = low
                at = k * NODES
                force_acc[at:at + NODES] += dot(loads[at:at + NODES], beside, NT)

        for q in range(PER_GROUP // 4):
            s = [sampled[q * 3 + i] for i in range(3)]
            j = g * PER_GROUP + q * 4
            back[source(j)] = s[0]
            back[source(j + 1)] = pltpu.roll(jnp.where(lane4 >= 96, s[0], s[1]), 32, 1)
            back[source(j + 2)] = pltpu.roll(jnp.where(lane4 >= 64, s[1], s[2]), 64, 1)
            back[source(j + 3)] = pltpu.roll(s[2], 96, 1)

        @pl.when(g > 0)
        def _():
            homeward(g * PER_GROUP).start()

        for i in range(1, PER_GROUP):
            homeward(g * PER_GROUP + i).start()

    got[me] = back[me]
    arrived(got, DEVICES - 1, back_recv)
    got_out[...] = got[...]
    arrived(recv, DEVICES - 1, send_sem)
    arrived(got, DEVICES - 1, back_send)


def finish(positions, got, slot, force_acc, moved, out, table):
    for k in range(3):
        both = jnp.concatenate(
            [got[pl.ds(0, HALF, stride=2), k, :], got[pl.ds(1, HALF, stride=2), k, :]], axis=1
        )
        high, low = split(both)
        table[k * HALF:(k + 1) * HALF, :COLS] = high
        table[k * HALF:(k + 1) * HALF, COLS:] = low

    @pl.loop(0, ROWS, unroll=4)
    def _(r):
        p = slot[pl.ds(r, 1), :]
        low = one_hot(jnp.bitwise_and(p, 255), 256)
        hit = jnp.broadcast_to(lax.shift_right_logical(p, 8), (HALF, COLS)) == iota((HALF, COLS), 0)
        g = dot(table[...], jnp.concatenate([low, low], axis=0))
        for k in range(3):
            mine = jnp.sum(jnp.where(hit, g[k * HALF:(k + 1) * HALF], 0.0), axis=0, keepdims=True)
            moved[k, pl.ds(r, 1), :] = positions[k, pl.ds(r, 1), :] + time_step * mine

    for k in range(3):
        out[k] = jnp.transpose(force_acc[k * NODES:(k + 1) * NODES])


def local(velocity, positions, stiff_h, stiff_v, marker_owner, marker_element, marker_coords):
    markers = ROWS * COLS
    group_tiles = PER_GROUP * CAP // LANES
    vmem = pl.BlockSpec(memory_space=pltpu.VMEM)
    got, slot, force_acc = pl.pallas_call(
        step,
        out_shape=(
            jax.ShapeDtypeStruct((DEVICES, 4, LANES), F32),
            jax.ShapeDtypeStruct((ROWS, COLS), I32),
            jax.ShapeDtypeStruct((3 * NODES, ELEMS), F32),
        ),
        in_specs=[vmem] * 6 + [pl.BlockSpec(memory_space=pl.ANY), vmem],
        out_specs=(vmem,) * 3,
        scratch_shapes=[
            pltpu.VMEM((4, ROWS + 16, COLS), F32),
            pltpu.VMEM((2, 4, 8, COLS), F32),
            pltpu.VMEM((6, ROWS, COLS), F32),
            pltpu.VMEM((7 * HALF, COLS), F32),
            pltpu.VMEM((HALF, 16, LANES), F32),
            pltpu.VMEM((DEVICES, 8, LANES), F32),
            pltpu.VMEM((group_tiles, 8, LANES), F32),
            pltpu.VMEM((group_tiles, 4, LANES), F32),
            pltpu.VMEM((DEVICES, 4, LANES), F32),
            pltpu.VMEM((DEVICES, 4, LANES), F32),
            pltpu.VMEM((3, ELEMS, NODES), F32),
            pltpu.VMEM((3 * NODES, 2 * ELEMS), BF),
            pltpu.VMEM((3 * NODES, 2 * CHUNK), BF),
            pltpu.SemaphoreType.DMA,
            pltpu.SemaphoreType.DMA((4,)),
            pltpu.SemaphoreType.DMA((4,)),
            pltpu.SemaphoreType.DMA,
            pltpu.SemaphoreType.DMA((GROUPS,)),
            pltpu.SemaphoreType.DMA,
            pltpu.SemaphoreType.DMA,
        ],
        compiler_params=pltpu.CompilerParams(collective_id=0, has_side_effects=True),
        name="step",
    )(
        positions, stiff_h, stiff_v,
        marker_owner.reshape(1, markers), marker_element.reshape(1, markers), marker_coords,
        velocity, jnp.asarray(SCALE_OF),
    )
    return pl.pallas_call(
        finish,
        out_shape=(
            jax.ShapeDtypeStruct((3, ROWS, COLS), F32),
            jax.ShapeDtypeStruct((3, ELEMS, NODES), F32),
        ),
        in_specs=[vmem] * 4,
        out_specs=(vmem,) * 2,
        scratch_shapes=[pltpu.VMEM((3 * HALF, 2 * COLS), BF)],
        name="finish",
    )(positions, got, slot, force_acc)


def solution(mesh):
    return jax.shard_map(
        local,
        mesh=mesh,
        in_specs=(
            P(None, ("gx", "gy"), None),
            P(None, ("gx", "gy"), None),
            P(("gx", "gy"), None),
            P(("gx", "gy"), None),
            P(("gx", "gy"), None),
            P(("gx", "gy")),
            P(None, ("gx", "gy")),
        ),
        out_specs=(P(None, ("gx", "gy"), None), P(None, ("gx", "gy"), None)),
        check_vma=False,
    )
```

```python
import math

import jax
import jax.numpy as jnp
import numpy as np
from jax import lax
from jax.experimental import pallas as pl
from jax.experimental.pallas import tpu as pltpu
from jax.sharding import PartitionSpec as P

POINTS = 8
NODES = 512
ELEMS = 256
ROWS = 32
COLS = 256
DEVICES = 128
LANES = 128
HALF = 64
TILES = 96
CHUNK = 512
CHUNK_TILES = CHUNK // LANES
CAP = 96
GROUPS = 8
PER_GROUP = DEVICES // GROUPS
LAG = 2

bend_modulus = 0.05
time_step = 0.5

BF = jnp.bfloat16
F32 = jnp.float32
I32 = jnp.int32
NN = (((1,), (0,)), ((), ()))
NT = (((1,), (1,)), ((), ()))


def dot(a, b, dims=NN):
    return lax.dot_general(a, b, dims, preferred_element_type=F32)


def iota(shape, dim):
    return lax.broadcasted_iota(I32, shape, dim)


def one_hot(row, count):
    hit = jnp.broadcast_to(row, (count, row.shape[1])) == iota((count, row.shape[1]), 0)
    return jnp.where(hit, 1.0, 0.0).astype(BF)


def split(x):
    high = x.astype(BF)
    return high, (x - high.astype(F32)).astype(BF)


def basis_tables():
    nodes = -np.cos(np.pi * np.arange(POINTS, dtype=np.float64) / (POINTS - 1))
    nodes = nodes.astype(np.float32).astype(np.float64)
    scale = np.zeros((POINTS, POINTS))
    for j in range(POINTS):
        for i in range(POINTS):
            if i != j:
                scale[j, i] = 1.0 / (nodes[i] - nodes[j])
    scale = np.broadcast_to(scale[:, :, None], (POINTS, POINTS, LANES))
    return nodes, np.ascontiguousarray(scale, np.float32)


NODE_AT, SCALE_OF = basis_tables()


def basis(row, scale):
    n = row.shape[1]
    x = jnp.broadcast_to(row, (POINTS, n))
    which = iota((POINTS, n), 0)
    product = None
    for j in range(POINTS):
        s = jnp.concatenate([scale[j]] * (n // LANES), axis=1)
        factor = jnp.where(which == j, 1.0, (x - float(NODE_AT[j])) * s)
        product = factor if product is None else product * factor
    return product

LOGICAL = pl.DeviceIdType.LOGICAL


def each_other(body):
    whole = (DEVICES - 1) // 8 * 8
    pl.loop(1, 1 + whole, unroll=8)(body)
    for j in range(1 + whole, DEVICES):
        body(j)


def tile_rows(comp, first, value):
    return jnp.concatenate([comp[first + t, value:value + 1, :] for t in range(CHUNK_TILES)], axis=1)


def chunk_of(comp, first, scales):
    hot = one_hot(tile_rows(comp, first, 3).astype(I32), ELEMS)
    return (hot, *(basis(tile_rows(comp, first, i), scales) for i in range(3)))


def sample_chunk(comp, first, scales, vt, sampled, into):
    hot, along_r, along_s, along_t = chunk_of(comp, first, scales)
    stacked = jnp.concatenate([hot, hot], axis=0)
    for k in range(3):
        gk = dot(vt[k * NODES:(k + 1) * NODES, :], stacked)
        over_r = None
        for a in range(POINTS):
            term = gk[a * 64:(a + 1) * 64] * along_r[a:a + 1]
            over_r = term if over_r is None else over_r + term
        over_s = None
        for b in range(POINTS):
            term = over_r[b * 8:(b + 1) * 8] * along_s[b:b + 1]
            over_s = term if over_s is None else over_s + term
        mine = jnp.sum(over_s * along_t, axis=0, keepdims=True)
        for t in range(CHUNK_TILES):
            sampled[into + t, k:k + 1, :] = mine[:, t * LANES:(t + 1) * LANES]


def deposit_chunk(comp, push_comp, first, scales, loads, force_acc):
    hot, along_r, along_s, along_t = chunk_of(comp, first, scales)
    plane = jnp.concatenate([along_s[b:b + 1] * along_t for b in range(POINTS)], axis=0)
    beside = jnp.concatenate([hot, hot], axis=1)
    for k in range(3):
        push = along_r * tile_rows(push_comp, first, k)
        for a in range(POINTS):
            high, low = split(plane * push[a:a + 1])
            at = k * NODES + a * 64
            loads[at:at + 64, :CHUNK] = high
            loads[at:at + 64, CHUNK:] = low
        at = k * NODES
        force_acc[at:at + NODES] += dot(loads[at:at + NODES], beside, NT)


def forces(ext, stiff_h, vals):
    def rows(k, first, count):
        return ext[k, first + 8:first + 8 + count]

    sh = stiff_h[...]
    sh_left = pltpu.roll(sh, 1, 1)
    sv = rows(3, 0, ROWS)
    sv_below = rows(3, -1, ROWS)
    for k in range(3):
        mid = rows(k, 0, ROWS)
        pull = (
            sh * (pltpu.roll(mid, COLS - 1, 1) - mid)
            + sh_left * (pltpu.roll(mid, 1, 1) - mid)
            + sv * (rows(k, 1, ROWS) - mid)
            + sv_below * (rows(k, -1, ROWS) - mid)
        )

        def lap_at(first):
            m = rows(k, first, ROWS)
            return (
                rows(k, first + 1, ROWS)
                + rows(k, first - 1, ROWS)
                + pltpu.roll(m, 1, 1)
                + pltpu.roll(m, COLS - 1, 1)
                - 4.0 * m
            )

        lap = lap_at(0)
        bend = (
            lap_at(1)
            + lap_at(-1)
            + pltpu.roll(lap, 1, 1)
            + pltpu.roll(lap, COLS - 1, 1)
            - 4.0 * lap
        )
        force = pull - bend_modulus * bend
        high = force.astype(BF).astype(F32)
        vals[2 * k] = high
        vals[2 * k + 1] = force - high


def step(positions_in, stiff_h_in, stiff_v_in, owner_in, element_in, coords_in, velocity, scale,
         got_out, slot, force_out,
         positions, stiff_h, stiff_v, owner, element, coords, force_acc,
         ext, halo, vals, acc, send, recv, push_send, push_recv, comp, push_comp, sampled, back, got,
         vel, vt, loads,
         in_sems, out_sem, vel_sem, halo_send, halo_recv, send_sem, recv_sem, push_send_sem, push_recv_sem,
         back_send, back_recv):
    me = lax.axis_index("gx") * 4 + lax.axis_index("gy")
    up, down = lax.rem(me + 1, DEVICES), lax.rem(me + DEVICES - 1, DEVICES)
    barrier = pltpu.get_barrier_semaphore()

    ins = [
        pltpu.make_async_copy(src, dst, in_sems.at[i])
        for i, (src, dst) in enumerate((
            (owner_in, owner), (positions_in, positions), (stiff_v_in, stiff_v),
            (coords_in, coords), (element_in, element), (stiff_h_in, stiff_h),
        ))
    ]
    for copy in ins:
        copy.start()
    fetch = pltpu.make_async_copy(velocity, vel, vel_sem)
    fetch.start()

    @each_other
    def _(j):
        pl.semaphore_signal(
            barrier, inc=1, device_id=lax.rem(me + j, DEVICES), device_id_type=LOGICAL
        )

    ins[0].wait()

    before = jnp.where(iota((COLS, COLS), 0) < iota((COLS, COLS), 1), 1.0, 0.0).astype(BF)
    counting = jnp.concatenate([before, jnp.ones((COLS, LANES), BF)], axis=1)

    def rank_rows(r, base):
        own = owner[:, pl.ds(pl.multiple_of(r * COLS, COLS), COLS)]
        hit = jnp.broadcast_to(own, (DEVICES, COLS)) == iota((DEVICES, COLS), 0)
        p = dot(jnp.where(hit, 1.0, 0.0).astype(BF), counting)
        both = jnp.concatenate([base, base], axis=1)
        rank = jnp.sum(jnp.where(hit, p[:, :COLS] + both, 0.0), axis=0, keepdims=True)
        slot[pl.ds(r, 1), :] = own * LANES + rank.astype(I32)
        return base + p[:, COLS:]

    lax.fori_loop(0, ROWS, rank_rows, jnp.zeros((DEVICES, LANES), F32), unroll=4)

    fetch.wait()
    for k in range(3):
        high, low = split(jnp.transpose(vel[k]))
        vt[k * NODES:(k + 1) * NODES, :ELEMS] = high
        vt[k * NODES:(k + 1) * NODES, ELEMS:] = low

    for copy in ins[1:]:
        copy.wait()
    pl.semaphore_wait(barrier, DEVICES - 1)

    last, lead = pl.ds(ROWS - 8, 8), pl.ds(0, 8)
    edge_copies = []
    for i, (target, side, part) in enumerate(((up, 0, last), (down, 1, lead))):
        for src, dst, n in (
            (positions.at[:, part, :], halo.at[side, pl.ds(0, 3)], 2 * i),
            (stiff_v.at[part, :], halo.at[side, 3], 2 * i + 1),
        ):
            edge_copies.append(
                pltpu.make_async_remote_copy(
                    src_ref=src,
                    dst_ref=dst,
                    send_sem=halo_send.at[n],
                    recv_sem=halo_recv.at[n],
                    device_id=target,
                    device_id_type=LOGICAL,
                )
            )
    for copy in edge_copies:
        copy.start()

    def spread(values, lows, whole, to):
        count = len(lows)
        total = 2 * count + whole
        acc[:total * HALF] = jnp.zeros((total * HALF, COLS), F32)

        @pl.loop(0, ROWS // 2, unroll=4)
        def _(h):
            r = h * 2
            p = jnp.concatenate([slot[pl.ds(r, 1), :], slot[pl.ds(r + 1, 1), :]], axis=1)
            low_hot = one_hot(jnp.bitwise_and(p, 255), 256)
            shape = (HALF, 2 * COLS)
            hit = jnp.broadcast_to(lax.shift_right_logical(p, 8), shape) == iota(shape, 0)
            picked = [
                jnp.where(hit, jnp.broadcast_to(row, shape), 0.0).astype(BF) for row in values(h)
            ]
            acc[:total * HALF] += dot(jnp.concatenate(picked, axis=0), low_hot, NT)

        for i in range(count + whole):
            v = acc[i * HALF:(i + 1) * HALF]
            if i < count:
                n = count + whole + i
                v = v + acc[n * HALF:(n + 1) * HALF]
            to[pl.ds(0, HALF, stride=2), i, :] = v[:, :LANES]
            to[pl.ds(1, HALF, stride=2), i, :] = v[:, LANES:]

    def place_rows(h):
        at = pl.ds(pl.multiple_of(h * 2 * COLS, 2 * COLS), 2 * COLS)
        rows = [coords[k:k + 1, at] for k in range(3)]
        highs = [row.astype(BF).astype(F32) for row in rows]
        return highs + [element[:, at].astype(F32)] + [r - h for r, h in zip(rows, highs)]

    def push_rows(h):
        def both(i):
            return jnp.concatenate([vals[i, pl.ds(h * 2, 1), :], vals[i, pl.ds(h * 2 + 1, 1), :]], axis=1)

        return [both(2 * k) for k in range(3)] + [both(2 * k + 1) for k in range(3)]

    spread(place_rows, (0, 1, 2), 1, send)

    def outward(j, src, dst, sent, landed):
        t = lax.rem(me + j, DEVICES)
        return pltpu.make_async_remote_copy(
            src_ref=src.at[t],
            dst_ref=dst.at[me],
            send_sem=sent,
            recv_sem=landed.at[lax.div(j, PER_GROUP)],
            device_id=t,
            device_id_type=LOGICAL,
        )

    def source(j):
        return lax.rem(me + DEVICES - j, DEVICES)

    def homeward(j):
        t = source(j)
        return pltpu.make_async_remote_copy(
            src_ref=back.at[t],
            dst_ref=got.at[me],
            send_sem=back_send,
            recv_sem=back_recv,
            device_id=t,
            device_id_type=LOGICAL,
        )

    def arrived(ref, count, sem):
        part = ref.at[pl.ds(0, count)]
        pltpu.make_async_copy(part, part, sem).wait()

    @each_other
    def _(j):
        outward(j, send, recv, send_sem, recv_sem).start()

    recv[me] = send[me]

    ext[:, 8:8 + ROWS] = jnp.concatenate([positions[...], stiff_v[...][None]], axis=0)
    for copy in edge_copies:
        copy.wait()
    ext[:, 6:8] = halo[0, :, 6:8, :]
    ext[:, 8 + ROWS:10 + ROWS] = halo[1, :, 0:2, :]
    forces(ext, stiff_h, vals)
    push_send[:, 3, :] = jnp.zeros((DEVICES, LANES), F32)
    spread(push_rows, (0, 1, 2), 0, push_send)

    @each_other
    def _(j):
        outward(j, push_send, push_recv, push_send_sem, push_recv_sem).start()

    push_recv[me] = push_send[me]

    force_acc[...] = jnp.zeros_like(force_acc)
    sampled[...] = jnp.zeros_like(sampled)
    scales = scale[...]
    lane4 = iota((4, LANES), 1)
    tiles = PER_GROUP * CAP // LANES
    chunks = PER_GROUP * CAP // CHUNK

    def pack(g, blocks, packed):
        for q in range(PER_GROUP // 4):
            b = [blocks[source(g * PER_GROUP + q * 4 + i)] for i in range(4)]
            r1 = pltpu.roll(b[1], 96, 1)
            r2 = pltpu.roll(b[2], 64, 1)
            r3 = pltpu.roll(b[3], 32, 1)
            at = g * tiles + q * 3
            packed[at] = jnp.where(lane4 < 96, b[0], r1)
            packed[at + 1] = jnp.where(lane4 < 64, r1, r2)
            packed[at + 2] = jnp.where(lane4 < 32, r2, r3)

    def send_back(g, own):
        for q in range(PER_GROUP // 4):
            s = [sampled[q * 3 + i] for i in range(3)]
            j = g * PER_GROUP + q * 4
            back[source(j)] = s[0]
            back[source(j + 1)] = pltpu.roll(jnp.where(lane4 >= 96, s[0], s[1]), 32, 1)
            back[source(j + 2)] = pltpu.roll(jnp.where(lane4 >= 64, s[1], s[2]), 64, 1)
            back[source(j + 3)] = pltpu.roll(s[2], 96, 1)
        for i in range(1 if own else 0, PER_GROUP):
            homeward(g * PER_GROUP + i).start()

    def sample_group(g):
        @pl.loop(0, chunks)
        def _(c):
            at = c * CHUNK_TILES
            sample_chunk(comp, g * tiles + at, scales, vt, sampled, at)

    arrived(recv, PER_GROUP - 1, recv_sem.at[0])
    pack(0, recv, comp)
    sample_group(0)
    send_back(0, True)
    got[me] = back[me]

    @pl.loop(1, LAG)
    def _(g):
        arrived(recv, PER_GROUP, recv_sem.at[g])
        pack(g, recv, comp)
        sample_group(g)
        send_back(g, False)

    arrived(push_recv, PER_GROUP - 1, push_recv_sem.at[0])
    pack(0, push_recv, push_comp)

    @pl.loop(LAG, GROUPS)
    def _(g):
        arrived(recv, PER_GROUP, recv_sem.at[g])
        pack(g, recv, comp)

        @pl.loop(0, chunks)
        def _(c):
            at = c * CHUNK_TILES
            sample_chunk(comp, g * tiles + at, scales, vt, sampled, at)
            deposit_chunk(comp, push_comp, (g - LAG) * tiles + at, scales, loads, force_acc)

        send_back(g, False)
        arrived(push_recv, PER_GROUP, push_recv_sem.at[g - LAG + 1])
        pack(g - LAG + 1, push_recv, push_comp)

    @pl.loop(GROUPS - LAG, GROUPS)
    def _(g):
        @pl.loop(0, chunks)
        def _(c):
            deposit_chunk(comp, push_comp, g * tiles + c * CHUNK_TILES, scales, loads, force_acc)

        @pl.when(g < GROUPS - 1)
        def _():
            arrived(push_recv, PER_GROUP, push_recv_sem.at[g + 1])
            pack(g + 1, push_recv, push_comp)

    flush = pltpu.make_async_copy(force_acc, force_out, out_sem)
    flush.start()
    arrived(got, DEVICES - 1, back_recv)
    got_out[...] = got[...]
    arrived(recv, DEVICES - 1, send_sem)
    arrived(recv, DEVICES - 1, push_send_sem)
    arrived(got, DEVICES - 1, back_send)
    flush.wait()


def finish(positions, got, slot, force_in, moved, out, table, force_acc, turned, in_sem, out_sem):
    ins, outs = [], []
    for k in range(3):
        part = pl.ds(k * NODES, NODES)
        ins.append(pltpu.make_async_copy(force_in.at[part], force_acc.at[part], in_sem.at[k]))
        outs.append(pltpu.make_async_copy(turned.at[k], out.at[k], out_sem.at[k]))
    for copy in ins:
        copy.start()
    for k in range(3):
        both = jnp.concatenate(
            [got[pl.ds(0, HALF, stride=2), k, :], got[pl.ds(1, HALF, stride=2), k, :]], axis=1
        )
        high, low = split(both)
        table[k * HALF:(k + 1) * HALF, :COLS] = high
        table[k * HALF:(k + 1) * HALF, COLS:] = low

    @pl.loop(0, ROWS, unroll=4)
    def _(r):
        p = slot[pl.ds(r, 1), :]
        low = one_hot(jnp.bitwise_and(p, 255), 256)
        hit = jnp.broadcast_to(lax.shift_right_logical(p, 8), (HALF, COLS)) == iota((HALF, COLS), 0)
        g = dot(table[...], jnp.concatenate([low, low], axis=0))
        for k in range(3):
            mine = jnp.sum(jnp.where(hit, g[k * HALF:(k + 1) * HALF], 0.0), axis=0, keepdims=True)
            moved[k, pl.ds(r, 1), :] = positions[k, pl.ds(r, 1), :] + time_step * mine

    for k in range(3):
        ins[k].wait()
        turned[k] = jnp.transpose(force_acc[k * NODES:(k + 1) * NODES])
        outs[k].start()
    for copy in outs:
        copy.wait()


def local(velocity, positions, stiff_h, stiff_v, marker_owner, marker_element, marker_coords):
    markers = ROWS * COLS
    group_tiles = PER_GROUP * CAP // LANES
    vmem = pl.BlockSpec(memory_space=pltpu.VMEM)
    got, slot, force_acc = pl.pallas_call(
        step,
        out_shape=(
            jax.ShapeDtypeStruct((DEVICES, 4, LANES), F32),
            jax.ShapeDtypeStruct((ROWS, COLS), I32),
            jax.ShapeDtypeStruct((3 * NODES, ELEMS), F32),
        ),
        in_specs=[pl.BlockSpec(memory_space=pl.ANY)] * 7 + [vmem],
        out_specs=(vmem, vmem, pl.BlockSpec(memory_space=pl.ANY)),
        scratch_shapes=[
            pltpu.VMEM((3, ROWS, COLS), F32),
            pltpu.VMEM((ROWS, COLS), F32),
            pltpu.VMEM((ROWS, COLS), F32),
            pltpu.VMEM((1, markers), I32),
            pltpu.VMEM((1, markers), I32),
            pltpu.VMEM((3, markers), F32),
            pltpu.VMEM((3 * NODES, ELEMS), F32),
            pltpu.VMEM((4, ROWS + 16, COLS), F32),
            pltpu.VMEM((2, 4, 8, COLS), F32),
            pltpu.VMEM((6, ROWS, COLS), F32),
            pltpu.VMEM((7 * HALF, COLS), F32),
            pltpu.VMEM((DEVICES, 4, LANES), F32),
            pltpu.VMEM((DEVICES, 4, LANES), F32),
            pltpu.VMEM((DEVICES, 4, LANES), F32),
            pltpu.VMEM((DEVICES, 4, LANES), F32),
            pltpu.VMEM((TILES, 4, LANES), F32),
            pltpu.VMEM((TILES, 4, LANES), F32),
            pltpu.VMEM((group_tiles, 4, LANES), F32),
            pltpu.VMEM((DEVICES, 4, LANES), F32),
            pltpu.VMEM((DEVICES, 4, LANES), F32),
            pltpu.VMEM((3, ELEMS, NODES), F32),
            pltpu.VMEM((3 * NODES, 2 * ELEMS), BF),
            pltpu.VMEM((3 * NODES, 2 * CHUNK), BF),
            pltpu.SemaphoreType.DMA((6,)),
            pltpu.SemaphoreType.DMA,
            pltpu.SemaphoreType.DMA,
            pltpu.SemaphoreType.DMA((4,)),
            pltpu.SemaphoreType.DMA((4,)),
            pltpu.SemaphoreType.DMA,
            pltpu.SemaphoreType.DMA((GROUPS,)),
            pltpu.SemaphoreType.DMA,
            pltpu.SemaphoreType.DMA((GROUPS,)),
            pltpu.SemaphoreType.DMA,
            pltpu.SemaphoreType.DMA,
        ],
        compiler_params=pltpu.CompilerParams(collective_id=0, has_side_effects=True),
        name="step",
    )(
        positions, stiff_h, stiff_v,
        marker_owner.reshape(1, markers), marker_element.reshape(1, markers), marker_coords,
        velocity, jnp.asarray(SCALE_OF),
    )
    return pl.pallas_call(
        finish,
        out_shape=(
            jax.ShapeDtypeStruct((3, ROWS, COLS), F32),
            jax.ShapeDtypeStruct((3, ELEMS, NODES), F32),
        ),
        in_specs=[vmem] * 3 + [pl.BlockSpec(memory_space=pl.ANY)],
        out_specs=(vmem, pl.BlockSpec(memory_space=pl.ANY)),
        scratch_shapes=[
            pltpu.VMEM((3 * HALF, 2 * COLS), BF),
            pltpu.VMEM((3 * NODES, ELEMS), F32),
            pltpu.VMEM((3, ELEMS, NODES), F32),
            pltpu.SemaphoreType.DMA((3,)),
            pltpu.SemaphoreType.DMA((3,)),
        ],
        name="finish",
    )(positions, got, slot, force_acc)


def solution(mesh):
    return jax.shard_map(
        local,
        mesh=mesh,
        in_specs=(
            P(None, ("gx", "gy"), None),
            P(None, ("gx", "gy"), None),
            P(("gx", "gy"), None),
            P(("gx", "gy"), None),
            P(("gx", "gy"), None),
            P(("gx", "gy")),
            P(None, ("gx", "gy")),
        ),
        out_specs=(P(None, ("gx", "gy"), None), P(None, ("gx", "gy"), None)),
        check_vma=False,
    )
```

```python
import math

import jax
import jax.numpy as jnp
import numpy as np
from jax import lax
from jax.experimental import pallas as pl
from jax.experimental.pallas import tpu as pltpu
from jax.sharding import PartitionSpec as P

POINTS = 8
NODES = 512
ELEMS = 256
ROWS = 32
COLS = 256
DEVICES = 128
LANES = 128
HALF = 64
TILES = 96
CHUNK = 512
CHUNK_TILES = CHUNK // LANES
CAP = 96
GROUPS = 8
PER_GROUP = DEVICES // GROUPS
LAG = 2
EARLY = 8

bend_modulus = 0.05
time_step = 0.5

BF = jnp.bfloat16
F32 = jnp.float32
I32 = jnp.int32
NN = (((1,), (0,)), ((), ()))
NT = (((1,), (1,)), ((), ()))


def dot(a, b, dims=NN):
    return lax.dot_general(a, b, dims, preferred_element_type=F32)


def iota(shape, dim):
    return lax.broadcasted_iota(I32, shape, dim)


def one_hot(row, count):
    hit = jnp.broadcast_to(row, (count, row.shape[1])) == iota((count, row.shape[1]), 0)
    return jnp.where(hit, 1.0, 0.0).astype(BF)


def split(x):
    high = x.astype(BF)
    return high, (x - high.astype(F32)).astype(BF)


def basis_tables():
    nodes = -np.cos(np.pi * np.arange(POINTS, dtype=np.float64) / (POINTS - 1))
    nodes = nodes.astype(np.float32).astype(np.float64)
    scale = np.zeros((POINTS, POINTS))
    for j in range(POINTS):
        for i in range(POINTS):
            if i != j:
                scale[j, i] = 1.0 / (nodes[i] - nodes[j])
    scale = np.broadcast_to(scale[:, :, None], (POINTS, POINTS, LANES))
    return nodes, np.ascontiguousarray(scale, np.float32)


NODE_AT, SCALE_OF = basis_tables()


def basis(row, scale):
    n = row.shape[1]
    x = jnp.broadcast_to(row, (POINTS, n))
    which = iota((POINTS, n), 0)
    product = None
    for j in range(POINTS):
        s = jnp.concatenate([scale[j]] * (n // LANES), axis=1)
        factor = jnp.where(which == j, 1.0, (x - float(NODE_AT[j])) * s)
        product = factor if product is None else product * factor
    return product

LOGICAL = pl.DeviceIdType.LOGICAL


def each_other(body):
    whole = (DEVICES - 1) // 8 * 8
    pl.loop(1, 1 + whole, unroll=8)(body)
    for j in range(1 + whole, DEVICES):
        body(j)


def tile_rows(comp, first, value):
    return jnp.concatenate([comp[first + t, value:value + 1, :] for t in range(CHUNK_TILES)], axis=1)


def chunk_of(comp, first, scales):
    hot = one_hot(tile_rows(comp, first, 3).astype(I32), ELEMS)
    return (hot, *(basis(tile_rows(comp, first, i), scales) for i in range(3)))


def sample_chunk(comp, first, scales, vt, sampled, into):
    hot, along_r, along_s, along_t = chunk_of(comp, first, scales)
    stacked = jnp.concatenate([hot, hot], axis=0)
    for k in range(3):
        gk = dot(vt[k * NODES:(k + 1) * NODES, :], stacked)
        over_r = None
        for a in range(POINTS):
            term = gk[a * 64:(a + 1) * 64] * along_r[a:a + 1]
            over_r = term if over_r is None else over_r + term
        over_s = None
        for b in range(POINTS):
            term = over_r[b * 8:(b + 1) * 8] * along_s[b:b + 1]
            over_s = term if over_s is None else over_s + term
        mine = jnp.sum(over_s * along_t, axis=0, keepdims=True)
        for t in range(CHUNK_TILES):
            sampled[into + t, k:k + 1, :] = mine[:, t * LANES:(t + 1) * LANES]


def deposit_chunk(comp, push_comp, first, scales, loads, force_acc):
    hot, along_r, along_s, along_t = chunk_of(comp, first, scales)
    plane = jnp.concatenate([along_s[b:b + 1] * along_t for b in range(POINTS)], axis=0)
    beside = jnp.concatenate([hot, hot], axis=1)
    for k in range(3):
        push = along_r * tile_rows(push_comp, first, k)
        for a in range(POINTS):
            high, low = split(plane * push[a:a + 1])
            at = k * NODES + a * 64
            loads[at:at + 64, :CHUNK] = high
            loads[at:at + 64, CHUNK:] = low
        at = k * NODES
        force_acc[at:at + NODES] += dot(loads[at:at + NODES], beside, NT)


def forces(ext, stiff_h, vals):
    def rows(k, first, count):
        return ext[k, first + 8:first + 8 + count]

    sh = stiff_h[...]
    sh_left = pltpu.roll(sh, 1, 1)
    sv = rows(3, 0, ROWS)
    sv_below = rows(3, -1, ROWS)
    for k in range(3):
        mid = rows(k, 0, ROWS)
        pull = (
            sh * (pltpu.roll(mid, COLS - 1, 1) - mid)
            + sh_left * (pltpu.roll(mid, 1, 1) - mid)
            + sv * (rows(k, 1, ROWS) - mid)
            + sv_below * (rows(k, -1, ROWS) - mid)
        )

        def lap_at(first):
            m = rows(k, first, ROWS)
            return (
                rows(k, first + 1, ROWS)
                + rows(k, first - 1, ROWS)
                + pltpu.roll(m, 1, 1)
                + pltpu.roll(m, COLS - 1, 1)
                - 4.0 * m
            )

        lap = lap_at(0)
        bend = (
            lap_at(1)
            + lap_at(-1)
            + pltpu.roll(lap, 1, 1)
            + pltpu.roll(lap, COLS - 1, 1)
            - 4.0 * lap
        )
        force = pull - bend_modulus * bend
        high = force.astype(BF).astype(F32)
        vals[2 * k] = high
        vals[2 * k + 1] = force - high


def step(positions_in, stiff_h_in, stiff_v_in, owner_in, element_in, coords_in, velocity, scale,
         got_out, slot, force_out,
         positions, stiff_h, stiff_v, owner, element, coords, force_acc,
         ext, halo, vals, acc, send, recv, push_send, push_recv, comp, push_comp, sampled, back, got,
         vel, vt, loads,
         in_sems, out_sem, vel_sem, halo_send, halo_recv, send_sem, recv_sem, push_send_sem, push_recv_sem,
         back_send, back_recv):
    me = lax.axis_index("gx") * 4 + lax.axis_index("gy")
    up, down = lax.rem(me + 1, DEVICES), lax.rem(me + DEVICES - 1, DEVICES)
    barrier = pltpu.get_barrier_semaphore()

    ins = [
        pltpu.make_async_copy(src, dst, in_sems.at[i])
        for i, (src, dst) in enumerate((
            (owner_in, owner), (positions_in, positions), (stiff_v_in, stiff_v),
            (coords_in, coords), (element_in, element), (stiff_h_in, stiff_h),
        ))
    ]
    for copy in ins:
        copy.start()
    fetch = pltpu.make_async_copy(velocity, vel, vel_sem)
    fetch.start()

    @each_other
    def _(j):
        pl.semaphore_signal(
            barrier, inc=1, device_id=lax.rem(me + j, DEVICES), device_id_type=LOGICAL
        )

    ins[0].wait()

    before = jnp.where(iota((COLS, COLS), 0) < iota((COLS, COLS), 1), 1.0, 0.0).astype(BF)
    counting = jnp.concatenate([before, jnp.ones((COLS, LANES), BF)], axis=1)

    def rank_rows(r, base):
        own = owner[:, pl.ds(pl.multiple_of(r * COLS, COLS), COLS)]
        hit = jnp.broadcast_to(own, (DEVICES, COLS)) == iota((DEVICES, COLS), 0)
        p = dot(jnp.where(hit, 1.0, 0.0).astype(BF), counting)
        both = jnp.concatenate([base, base], axis=1)
        rank = jnp.sum(jnp.where(hit, p[:, :COLS] + both, 0.0), axis=0, keepdims=True)
        slot[pl.ds(r, 1), :] = own * LANES + rank.astype(I32)
        return base + p[:, COLS:]

    lax.fori_loop(0, ROWS, rank_rows, jnp.zeros((DEVICES, LANES), F32), unroll=8)

    fetch.wait()
    for k in range(3):
        high, low = split(jnp.transpose(vel[k]))
        vt[k * NODES:(k + 1) * NODES, :ELEMS] = high
        vt[k * NODES:(k + 1) * NODES, ELEMS:] = low

    for copy in ins[1:]:
        copy.wait()
    pl.semaphore_wait(barrier, DEVICES - 1)

    last, lead = pl.ds(ROWS - 8, 8), pl.ds(0, 8)
    edge_copies = []
    for i, (target, side, part) in enumerate(((up, 0, last), (down, 1, lead))):
        for src, dst, n in (
            (positions.at[:, part, :], halo.at[side, pl.ds(0, 3)], 2 * i),
            (stiff_v.at[part, :], halo.at[side, 3], 2 * i + 1),
        ):
            edge_copies.append(
                pltpu.make_async_remote_copy(
                    src_ref=src,
                    dst_ref=dst,
                    send_sem=halo_send.at[n],
                    recv_sem=halo_recv.at[n],
                    device_id=target,
                    device_id_type=LOGICAL,
                )
            )
    for copy in edge_copies:
        copy.start()

    def spread(values, lows, whole, to):
        count = len(lows)
        total = 2 * count + whole
        acc[:total * HALF] = jnp.zeros((total * HALF, COLS), F32)

        @pl.loop(0, ROWS // 2, unroll=8)
        def _(h):
            r = h * 2
            p = jnp.concatenate([slot[pl.ds(r, 1), :], slot[pl.ds(r + 1, 1), :]], axis=1)
            low_hot = one_hot(jnp.bitwise_and(p, 255), 256)
            shape = (HALF, 2 * COLS)
            hit = jnp.broadcast_to(lax.shift_right_logical(p, 8), shape) == iota(shape, 0)
            picked = [
                jnp.where(hit, jnp.broadcast_to(row, shape), 0.0).astype(BF) for row in values(h)
            ]
            acc[:total * HALF] += dot(jnp.concatenate(picked, axis=0), low_hot, NT)

        for i in range(count + whole):
            v = acc[i * HALF:(i + 1) * HALF]
            if i < count:
                n = count + whole + i
                v = v + acc[n * HALF:(n + 1) * HALF]
            to[pl.ds(0, HALF, stride=2), i, :] = v[:, :LANES]
            to[pl.ds(1, HALF, stride=2), i, :] = v[:, LANES:]

    def place_rows(h):
        at = pl.ds(pl.multiple_of(h * 2 * COLS, 2 * COLS), 2 * COLS)
        rows = [coords[k:k + 1, at] for k in range(3)]
        highs = [row.astype(BF).astype(F32) for row in rows]
        return highs + [element[:, at].astype(F32)] + [r - h for r, h in zip(rows, highs)]

    def push_rows(h):
        def both(i):
            return jnp.concatenate([vals[i, pl.ds(h * 2, 1), :], vals[i, pl.ds(h * 2 + 1, 1), :]], axis=1)

        return [both(2 * k) for k in range(3)] + [both(2 * k + 1) for k in range(3)]

    spread(place_rows, (0, 1, 2), 1, send)

    def outward(j, src, dst, sent, landed):
        t = lax.rem(me + j, DEVICES)
        return pltpu.make_async_remote_copy(
            src_ref=src.at[t],
            dst_ref=dst.at[me],
            send_sem=sent,
            recv_sem=landed.at[lax.div(j, PER_GROUP)],
            device_id=t,
            device_id_type=LOGICAL,
        )

    def source(j):
        return lax.rem(me + DEVICES - j, DEVICES)

    def homeward(j):
        t = source(j)
        return pltpu.make_async_remote_copy(
            src_ref=back.at[t],
            dst_ref=got.at[me],
            send_sem=back_send,
            recv_sem=back_recv,
            device_id=t,
            device_id_type=LOGICAL,
        )

    def arrived(ref, count, sem):
        part = ref.at[pl.ds(0, count)]
        pltpu.make_async_copy(part, part, sem).wait()

    @each_other
    def _(j):
        outward(j, send, recv, send_sem, recv_sem).start()

    recv[me] = send[me]

    ext[:, 8:8 + ROWS] = jnp.concatenate([positions[...], stiff_v[...][None]], axis=0)
    for copy in edge_copies:
        copy.wait()
    ext[:, 6:8] = halo[0, :, 6:8, :]
    ext[:, 8 + ROWS:10 + ROWS] = halo[1, :, 0:2, :]
    forces(ext, stiff_h, vals)
    push_send[:, 3, :] = jnp.zeros((DEVICES, LANES), F32)
    spread(push_rows, (0, 1, 2), 0, push_send)

    @each_other
    def _(j):
        outward(j, push_send, push_recv, push_send_sem, push_recv_sem).start()

    push_recv[me] = push_send[me]

    force_acc[...] = jnp.zeros_like(force_acc)
    sampled[...] = jnp.zeros_like(sampled)
    scales = scale[...]
    lane4 = iota((4, LANES), 1)
    tiles = PER_GROUP * CAP // LANES
    chunks = PER_GROUP * CAP // CHUNK

    def pack(g, blocks, packed):
        for q in range(PER_GROUP // 4):
            b = [blocks[source(g * PER_GROUP + q * 4 + i)] for i in range(4)]
            r1 = pltpu.roll(b[1], 96, 1)
            r2 = pltpu.roll(b[2], 64, 1)
            r3 = pltpu.roll(b[3], 32, 1)
            at = g * tiles + q * 3
            packed[at] = jnp.where(lane4 < 96, b[0], r1)
            packed[at + 1] = jnp.where(lane4 < 64, r1, r2)
            packed[at + 2] = jnp.where(lane4 < 32, r2, r3)

    def send_back(g, own):
        for q in range(PER_GROUP // 4):
            s = [sampled[q * 3 + i] for i in range(3)]
            j = g * PER_GROUP + q * 4
            back[source(j)] = s[0]
            back[source(j + 1)] = pltpu.roll(jnp.where(lane4 >= 96, s[0], s[1]), 32, 1)
            back[source(j + 2)] = pltpu.roll(jnp.where(lane4 >= 64, s[1], s[2]), 64, 1)
            back[source(j + 3)] = pltpu.roll(s[2], 96, 1)
        for i in range(1 if own else 0, PER_GROUP):
            homeward(g * PER_GROUP + i).start()

    def sample_group(g):
        @pl.loop(0, chunks)
        def _(c):
            at = c * CHUNK_TILES
            sample_chunk(comp, g * tiles + at, scales, vt, sampled, at)

    arrived(recv, PER_GROUP - 1, recv_sem.at[0])
    pack(0, recv, comp)
    sample_group(0)
    send_back(0, True)
    got[me] = back[me]

    @pl.loop(1, LAG)
    def _(g):
        arrived(recv, PER_GROUP, recv_sem.at[g])
        pack(g, recv, comp)
        sample_group(g)
        send_back(g, False)

    arrived(push_recv, PER_GROUP - 1, push_recv_sem.at[0])
    pack(0, push_recv, push_comp)

    @pl.loop(LAG, GROUPS)
    def _(g):
        arrived(recv, PER_GROUP, recv_sem.at[g])
        pack(g, recv, comp)

        @pl.loop(0, chunks)
        def _(c):
            at = c * CHUNK_TILES
            sample_chunk(comp, g * tiles + at, scales, vt, sampled, at)
            deposit_chunk(comp, push_comp, (g - LAG) * tiles + at, scales, loads, force_acc)

        send_back(g, False)
        arrived(push_recv, PER_GROUP, push_recv_sem.at[g - LAG + 1])
        pack(g - LAG + 1, push_recv, push_comp)

    @pl.loop(GROUPS - LAG, GROUPS)
    def _(g):
        @pl.loop(0, chunks)
        def _(c):
            deposit_chunk(comp, push_comp, g * tiles + c * CHUNK_TILES, scales, loads, force_acc)

        @pl.when(g < GROUPS - 1)
        def _():
            arrived(push_recv, PER_GROUP, push_recv_sem.at[g + 1])
            pack(g + 1, push_recv, push_comp)

    flush = pltpu.make_async_copy(force_acc, force_out, out_sem)
    flush.start()
    arrived(got, DEVICES - 1, back_recv)
    got_out[...] = got[...]
    arrived(recv, DEVICES - 1, send_sem)
    arrived(recv, DEVICES - 1, push_send_sem)
    arrived(got, DEVICES - 1, back_send)
    flush.wait()


def finish(positions, got, slot, force_in, moved, out, table, force_acc, turned, in_sem, out_sem):
    ins, outs = [], []
    for k in range(3):
        part = pl.ds(k * NODES, NODES)
        ins.append(pltpu.make_async_copy(force_in.at[part], force_acc.at[part], in_sem.at[k]))
        outs.append(pltpu.make_async_copy(turned.at[k], out.at[k], out_sem.at[k]))
    for copy in ins:
        copy.start()
    for k in range(3):
        both = jnp.concatenate(
            [got[pl.ds(0, HALF, stride=2), k, :], got[pl.ds(1, HALF, stride=2), k, :]], axis=1
        )
        high, low = split(both)
        table[k * HALF:(k + 1) * HALF, :COLS] = high
        table[k * HALF:(k + 1) * HALF, COLS:] = low

    def one_row(r):
        p = slot[pl.ds(r, 1), :]
        low = one_hot(jnp.bitwise_and(p, 255), 256)
        hit = jnp.broadcast_to(lax.shift_right_logical(p, 8), (HALF, COLS)) == iota((HALF, COLS), 0)
        g = dot(table[...], jnp.concatenate([low, low], axis=0))
        for k in range(3):
            mine = jnp.sum(jnp.where(hit, g[k * HALF:(k + 1) * HALF], 0.0), axis=0, keepdims=True)
            moved[k, pl.ds(r, 1), :] = positions[k, pl.ds(r, 1), :] + time_step * mine

    pl.loop(0, EARLY, unroll=4)(one_row)
    for k in range(3):
        ins[k].wait()
        turned[k] = jnp.transpose(force_acc[k * NODES:(k + 1) * NODES])
        outs[k].start()
    pl.loop(EARLY, ROWS, unroll=4)(one_row)
    for copy in outs:
        copy.wait()


def local(velocity, positions, stiff_h, stiff_v, marker_owner, marker_element, marker_coords):
    markers = ROWS * COLS
    group_tiles = PER_GROUP * CAP // LANES
    vmem = pl.BlockSpec(memory_space=pltpu.VMEM)
    got, slot, force_acc = pl.pallas_call(
        step,
        out_shape=(
            jax.ShapeDtypeStruct((DEVICES, 4, LANES), F32),
            jax.ShapeDtypeStruct((ROWS, COLS), I32),
            jax.ShapeDtypeStruct((3 * NODES, ELEMS), F32),
        ),
        in_specs=[pl.BlockSpec(memory_space=pl.ANY)] * 7 + [vmem],
        out_specs=(vmem, vmem, pl.BlockSpec(memory_space=pl.ANY)),
        scratch_shapes=[
            pltpu.VMEM((3, ROWS, COLS), F32),
            pltpu.VMEM((ROWS, COLS), F32),
            pltpu.VMEM((ROWS, COLS), F32),
            pltpu.VMEM((1, markers), I32),
            pltpu.VMEM((1, markers), I32),
            pltpu.VMEM((3, markers), F32),
            pltpu.VMEM((3 * NODES, ELEMS), F32),
            pltpu.VMEM((4, ROWS + 16, COLS), F32),
            pltpu.VMEM((2, 4, 8, COLS), F32),
            pltpu.VMEM((6, ROWS, COLS), F32),
            pltpu.VMEM((7 * HALF, COLS), F32),
            pltpu.VMEM((DEVICES, 4, LANES), F32),
            pltpu.VMEM((DEVICES, 4, LANES), F32),
            pltpu.VMEM((DEVICES, 4, LANES), F32),
            pltpu.VMEM((DEVICES, 4, LANES), F32),
            pltpu.VMEM((TILES, 4, LANES), F32),
            pltpu.VMEM((TILES, 4, LANES), F32),
            pltpu.VMEM((group_tiles, 4, LANES), F32),
            pltpu.VMEM((DEVICES, 4, LANES), F32),
            pltpu.VMEM((DEVICES, 4, LANES), F32),
            pltpu.VMEM((3, ELEMS, NODES), F32),
            pltpu.VMEM((3 * NODES, 2 * ELEMS), BF),
            pltpu.VMEM((3 * NODES, 2 * CHUNK), BF),
            pltpu.SemaphoreType.DMA((6,)),
            pltpu.SemaphoreType.DMA,
            pltpu.SemaphoreType.DMA,
            pltpu.SemaphoreType.DMA((4,)),
            pltpu.SemaphoreType.DMA((4,)),
            pltpu.SemaphoreType.DMA,
            pltpu.SemaphoreType.DMA((GROUPS,)),
            pltpu.SemaphoreType.DMA,
            pltpu.SemaphoreType.DMA((GROUPS,)),
            pltpu.SemaphoreType.DMA,
            pltpu.SemaphoreType.DMA,
        ],
        compiler_params=pltpu.CompilerParams(collective_id=0, has_side_effects=True),
        name="step",
    )(
        positions, stiff_h, stiff_v,
        marker_owner.reshape(1, markers), marker_element.reshape(1, markers), marker_coords,
        velocity, jnp.asarray(SCALE_OF),
    )
    return pl.pallas_call(
        finish,
        out_shape=(
            jax.ShapeDtypeStruct((3, ROWS, COLS), F32),
            jax.ShapeDtypeStruct((3, ELEMS, NODES), F32),
        ),
        in_specs=[vmem] * 3 + [pl.BlockSpec(memory_space=pl.ANY)],
        out_specs=(vmem, pl.BlockSpec(memory_space=pl.ANY)),
        scratch_shapes=[
            pltpu.VMEM((3 * HALF, 2 * COLS), BF),
            pltpu.VMEM((3 * NODES, ELEMS), F32),
            pltpu.VMEM((3, ELEMS, NODES), F32),
            pltpu.SemaphoreType.DMA((3,)),
            pltpu.SemaphoreType.DMA((3,)),
        ],
        name="finish",
    )(positions, got, slot, force_acc)


def solution(mesh):
    return jax.shard_map(
        local,
        mesh=mesh,
        in_specs=(
            P(None, ("gx", "gy"), None),
            P(None, ("gx", "gy"), None),
            P(("gx", "gy"), None),
            P(("gx", "gy"), None),
            P(("gx", "gy"), None),
            P(("gx", "gy")),
            P(None, ("gx", "gy")),
        ),
        out_specs=(P(None, ("gx", "gy"), None), P(None, ("gx", "gy"), None)),
        check_vma=False,
    )
```

```python
import math

import jax
import jax.numpy as jnp
import numpy as np
from jax import lax
from jax.experimental import pallas as pl
from jax.experimental.pallas import tpu as pltpu
from jax.sharding import PartitionSpec as P

POINTS = 8
NODES = 512
ELEMS = 256
ROWS = 32
COLS = 256
DEVICES = 128
LANES = 128
HALF = 64
TILES = 96
CHUNK = 512
CHUNK_TILES = CHUNK // LANES
CAP = 96
GROUPS = 8
PER_GROUP = DEVICES // GROUPS
LAG = 2
EARLY = 8

bend_modulus = 0.05
time_step = 0.5

BF = jnp.bfloat16
F32 = jnp.float32
I32 = jnp.int32
NN = (((1,), (0,)), ((), ()))
NT = (((1,), (1,)), ((), ()))


def dot(a, b, dims=NN):
    return lax.dot_general(a, b, dims, preferred_element_type=F32)


def iota(shape, dim):
    return lax.broadcasted_iota(I32, shape, dim)


def one_hot(row, count):
    hit = jnp.broadcast_to(row, (count, row.shape[1])) == iota((count, row.shape[1]), 0)
    return jnp.where(hit, 1.0, 0.0).astype(BF)


def split(x):
    high = x.astype(BF)
    return high, (x - high.astype(F32)).astype(BF)


def basis_tables():
    nodes = -np.cos(np.pi * np.arange(POINTS, dtype=np.float64) / (POINTS - 1))
    nodes = nodes.astype(np.float32).astype(np.float64)
    scale = np.zeros((POINTS, POINTS))
    for j in range(POINTS):
        for i in range(POINTS):
            if i != j:
                scale[j, i] = 1.0 / (nodes[i] - nodes[j])
    scale = np.broadcast_to(scale[:, :, None], (POINTS, POINTS, LANES))
    return nodes, np.ascontiguousarray(scale, np.float32)


NODE_AT, SCALE_OF = basis_tables()


def basis(row, scale):
    n = row.shape[1]
    x = jnp.broadcast_to(row, (POINTS, n))
    which = iota((POINTS, n), 0)
    product = None
    for j in range(POINTS):
        s = jnp.concatenate([scale[j]] * (n // LANES), axis=1)
        factor = jnp.where(which == j, 1.0, (x - float(NODE_AT[j])) * s)
        product = factor if product is None else product * factor
    return product

LOGICAL = pl.DeviceIdType.LOGICAL


def each_other(body):
    whole = (DEVICES - 1) // 8 * 8
    pl.loop(1, 1 + whole, unroll=8)(body)
    for j in range(1 + whole, DEVICES):
        body(j)


def tile_rows(comp, first, value):
    return jnp.concatenate([comp[first + t, value:value + 1, :] for t in range(CHUNK_TILES)], axis=1)


def chunk_of(comp, first, scales):
    hot = one_hot(tile_rows(comp, first, 3).astype(I32), ELEMS)
    return (hot, *(basis(tile_rows(comp, first, i), scales) for i in range(3)))


def sample_chunk(comp, first, scales, vt, sampled, into):
    hot, along_r, along_s, along_t = chunk_of(comp, first, scales)
    stacked = jnp.concatenate([hot, hot], axis=0)
    for k in range(3):
        gk = dot(vt[k * NODES:(k + 1) * NODES, :], stacked)
        over_r = None
        for a in range(POINTS):
            term = gk[a * 64:(a + 1) * 64] * along_r[a:a + 1]
            over_r = term if over_r is None else over_r + term
        over_s = None
        for b in range(POINTS):
            term = over_r[b * 8:(b + 1) * 8] * along_s[b:b + 1]
            over_s = term if over_s is None else over_s + term
        mine = jnp.sum(over_s * along_t, axis=0, keepdims=True)
        for t in range(CHUNK_TILES):
            sampled[into + t, k:k + 1, :] = mine[:, t * LANES:(t + 1) * LANES]


def deposit_chunk(comp, push_comp, first, scales, loads, force_acc):
    hot, along_r, along_s, along_t = chunk_of(comp, first, scales)
    plane = jnp.concatenate([along_s[b:b + 1] * along_t for b in range(POINTS)], axis=0)
    beside = jnp.concatenate([hot, hot], axis=1)
    for k in range(3):
        push = along_r * tile_rows(push_comp, first, k)
        for a in range(POINTS):
            high, low = split(plane * push[a:a + 1])
            at = k * NODES + a * 64
            loads[at:at + 64, :CHUNK] = high
            loads[at:at + 64, CHUNK:] = low
        at = k * NODES
        force_acc[at:at + NODES] += dot(loads[at:at + NODES], beside, NT)


def forces(ext, stiff_h, vals):
    def rows(k, first, count):
        return ext[k, first + 8:first + 8 + count]

    sh = stiff_h[...]
    sh_left = pltpu.roll(sh, 1, 1)
    sv = rows(3, 0, ROWS)
    sv_below = rows(3, -1, ROWS)
    for k in range(3):
        mid = rows(k, 0, ROWS)
        pull = (
            sh * (pltpu.roll(mid, COLS - 1, 1) - mid)
            + sh_left * (pltpu.roll(mid, 1, 1) - mid)
            + sv * (rows(k, 1, ROWS) - mid)
            + sv_below * (rows(k, -1, ROWS) - mid)
        )

        def lap_at(first):
            m = rows(k, first, ROWS)
            return (
                rows(k, first + 1, ROWS)
                + rows(k, first - 1, ROWS)
                + pltpu.roll(m, 1, 1)
                + pltpu.roll(m, COLS - 1, 1)
                - 4.0 * m
            )

        lap = lap_at(0)
        bend = (
            lap_at(1)
            + lap_at(-1)
            + pltpu.roll(lap, 1, 1)
            + pltpu.roll(lap, COLS - 1, 1)
            - 4.0 * lap
        )
        force = pull - bend_modulus * bend
        high = force.astype(BF).astype(F32)
        vals[2 * k] = high
        vals[2 * k + 1] = force - high


def step(positions_in, stiff_h_in, stiff_v_in, owner_in, element_in, coords_in, velocity, scale,
         got_out, slot, force_out,
         positions, stiff_h, stiff_v, owner, element, coords, force_acc,
         ext, halo, vals, acc, send, recv, push_send, push_recv, comp, push_comp, sampled, back, got,
         vel, vt, loads,
         in_sems, out_sem, vel_sem, halo_send, halo_recv, send_sem, recv_sem, push_send_sem, push_recv_sem,
         back_send, back_recv):
    me = lax.axis_index("gx") * 4 + lax.axis_index("gy")
    up, down = lax.rem(me + 1, DEVICES), lax.rem(me + DEVICES - 1, DEVICES)
    barrier = pltpu.get_barrier_semaphore()

    ins = [
        pltpu.make_async_copy(src, dst, in_sems.at[i])
        for i, (src, dst) in enumerate((
            (owner_in, owner), (positions_in, positions), (stiff_v_in, stiff_v),
            (coords_in, coords), (element_in, element), (stiff_h_in, stiff_h),
        ))
    ]
    for copy in ins:
        copy.start()
    fetch = pltpu.make_async_copy(velocity, vel, vel_sem)
    fetch.start()

    @each_other
    def _(j):
        pl.semaphore_signal(
            barrier, inc=1, device_id=lax.rem(me + j, DEVICES), device_id_type=LOGICAL
        )

    ins[0].wait()

    before = jnp.where(iota((COLS, COLS), 0) < iota((COLS, COLS), 1), 1.0, 0.0).astype(BF)
    counting = jnp.concatenate([before, jnp.ones((COLS, LANES), BF)], axis=1)

    def rank_rows(r, base):
        own = owner[:, pl.ds(pl.multiple_of(r * COLS, COLS), COLS)]
        hit = jnp.broadcast_to(own, (DEVICES, COLS)) == iota((DEVICES, COLS), 0)
        p = dot(jnp.where(hit, 1.0, 0.0).astype(BF), counting)
        both = jnp.concatenate([base, base], axis=1)
        rank = jnp.sum(jnp.where(hit, p[:, :COLS] + both, 0.0), axis=0, keepdims=True)
        slot[pl.ds(r, 1), :] = own * LANES + rank.astype(I32)
        return base + p[:, COLS:]

    lax.fori_loop(0, ROWS, rank_rows, jnp.zeros((DEVICES, LANES), F32), unroll=8)

    fetch.wait()
    for k in range(3):
        high, low = split(jnp.transpose(vel[k]))
        vt[k * NODES:(k + 1) * NODES, :ELEMS] = high
        vt[k * NODES:(k + 1) * NODES, ELEMS:] = low

    for copy in ins[1:]:
        copy.wait()
    pl.semaphore_wait(barrier, DEVICES - 1)

    last, lead = pl.ds(ROWS - 8, 8), pl.ds(0, 8)
    edge_copies = []
    for i, (target, side, part) in enumerate(((up, 0, last), (down, 1, lead))):
        for src, dst, n in (
            (positions.at[:, part, :], halo.at[side, pl.ds(0, 3)], 2 * i),
            (stiff_v.at[part, :], halo.at[side, 3], 2 * i + 1),
        ):
            edge_copies.append(
                pltpu.make_async_remote_copy(
                    src_ref=src,
                    dst_ref=dst,
                    send_sem=halo_send.at[n],
                    recv_sem=halo_recv.at[n],
                    device_id=target,
                    device_id_type=LOGICAL,
                )
            )
    for copy in edge_copies:
        copy.start()

    def spread(values, lows, whole, to):
        count = len(lows)
        total = 2 * count + whole
        acc[:total * HALF] = jnp.zeros((total * HALF, COLS), F32)

        @pl.loop(0, ROWS // 2, unroll=8)
        def _(h):
            r = h * 2
            p = jnp.concatenate([slot[pl.ds(r, 1), :], slot[pl.ds(r + 1, 1), :]], axis=1)
            low_hot = one_hot(jnp.bitwise_and(p, 255), 256)
            shape = (HALF, 2 * COLS)
            hit = jnp.broadcast_to(lax.shift_right_logical(p, 8), shape) == iota(shape, 0)
            picked = [
                jnp.where(hit, jnp.broadcast_to(row, shape), 0.0).astype(BF) for row in values(h)
            ]
            acc[:total * HALF] += dot(jnp.concatenate(picked, axis=0), low_hot, NT)

        for i in range(count + whole):
            v = acc[i * HALF:(i + 1) * HALF]
            if i < count:
                n = count + whole + i
                v = v + acc[n * HALF:(n + 1) * HALF]
            to[pl.ds(0, HALF, stride=2), i, :] = v[:, :LANES]
            to[pl.ds(1, HALF, stride=2), i, :] = v[:, LANES:]

    def place_rows(h):
        at = pl.ds(pl.multiple_of(h * 2 * COLS, 2 * COLS), 2 * COLS)
        rows = [coords[k:k + 1, at] for k in range(3)]
        highs = [row.astype(BF).astype(F32) for row in rows]
        return highs + [element[:, at].astype(F32)] + [r - h for r, h in zip(rows, highs)]

    def push_rows(h):
        def both(i):
            return jnp.concatenate([vals[i, pl.ds(h * 2, 1), :], vals[i, pl.ds(h * 2 + 1, 1), :]], axis=1)

        return [both(2 * k) for k in range(3)] + [both(2 * k + 1) for k in range(3)]

    spread(place_rows, (0, 1, 2), 1, send)

    def outward(j, src, dst, sent, landed):
        t = lax.rem(me + j, DEVICES)
        return pltpu.make_async_remote_copy(
            src_ref=src.at[t],
            dst_ref=dst.at[me],
            send_sem=sent,
            recv_sem=landed.at[lax.div(j, PER_GROUP)],
            device_id=t,
            device_id_type=LOGICAL,
        )

    def source(j):
        return lax.rem(me + DEVICES - j, DEVICES)

    def homeward(j):
        t = source(j)
        return pltpu.make_async_remote_copy(
            src_ref=back.at[t],
            dst_ref=got.at[me],
            send_sem=back_send,
            recv_sem=back_recv,
            device_id=t,
            device_id_type=LOGICAL,
        )

    def arrived(ref, count, sem):
        part = ref.at[pl.ds(0, count)]
        pltpu.make_async_copy(part, part, sem).wait()

    @each_other
    def _(j):
        outward(j, send, recv, send_sem, recv_sem).start()

    recv[me] = send[me]

    ext[:, 8:8 + ROWS] = jnp.concatenate([positions[...], stiff_v[...][None]], axis=0)
    for copy in edge_copies:
        copy.wait()
    ext[:, 6:8] = halo[0, :, 6:8, :]
    ext[:, 8 + ROWS:10 + ROWS] = halo[1, :, 0:2, :]
    forces(ext, stiff_h, vals)
    push_send[:, 3, :] = jnp.zeros((DEVICES, LANES), F32)
    spread(push_rows, (0, 1, 2), 0, push_send)

    @each_other
    def _(j):
        outward(j, push_send, push_recv, push_send_sem, push_recv_sem).start()

    push_recv[me] = push_send[me]

    force_acc[...] = jnp.zeros_like(force_acc)
    sampled[...] = jnp.zeros_like(sampled)
    scales = scale[...]
    lane4 = iota((4, LANES), 1)
    tiles = PER_GROUP * CAP // LANES
    chunks = PER_GROUP * CAP // CHUNK

    def pack(g, blocks, packed):
        for q in range(PER_GROUP // 4):
            b = [blocks[source(g * PER_GROUP + q * 4 + i)] for i in range(4)]
            r1 = pltpu.roll(b[1], 96, 1)
            r2 = pltpu.roll(b[2], 64, 1)
            r3 = pltpu.roll(b[3], 32, 1)
            at = g * tiles + q * 3
            packed[at] = jnp.where(lane4 < 96, b[0], r1)
            packed[at + 1] = jnp.where(lane4 < 64, r1, r2)
            packed[at + 2] = jnp.where(lane4 < 32, r2, r3)

    def send_back(g, own):
        for q in range(PER_GROUP // 4):
            s = [sampled[q * 3 + i] for i in range(3)]
            j = g * PER_GROUP + q * 4
            back[source(j)] = s[0]
            back[source(j + 1)] = pltpu.roll(jnp.where(lane4 >= 96, s[0], s[1]), 32, 1)
            back[source(j + 2)] = pltpu.roll(jnp.where(lane4 >= 64, s[1], s[2]), 64, 1)
            back[source(j + 3)] = pltpu.roll(s[2], 96, 1)
        for i in range(1 if own else 0, PER_GROUP):
            homeward(g * PER_GROUP + i).start()

    def sample_group(g):
        @pl.loop(0, chunks)
        def _(c):
            at = c * CHUNK_TILES
            sample_chunk(comp, g * tiles + at, scales, vt, sampled, at)

    arrived(recv, PER_GROUP - 1, recv_sem.at[0])
    pack(0, recv, comp)
    sample_group(0)
    send_back(0, True)
    got[me] = back[me]

    @pl.loop(1, LAG)
    def _(g):
        arrived(recv, PER_GROUP, recv_sem.at[g])
        pack(g, recv, comp)
        sample_group(g)
        send_back(g, False)

    arrived(push_recv, PER_GROUP - 1, push_recv_sem.at[0])
    pack(0, push_recv, push_comp)

    @pl.loop(LAG, GROUPS)
    def _(g):
        arrived(recv, PER_GROUP, recv_sem.at[g])
        pack(g, recv, comp)

        @pl.loop(0, chunks)
        def _(c):
            at = c * CHUNK_TILES
            sample_chunk(comp, g * tiles + at, scales, vt, sampled, at)
            deposit_chunk(comp, push_comp, (g - LAG) * tiles + at, scales, loads, force_acc)

        send_back(g, False)
        arrived(push_recv, PER_GROUP, push_recv_sem.at[g - LAG + 1])
        pack(g - LAG + 1, push_recv, push_comp)

    @pl.loop(GROUPS - LAG, GROUPS)
    def _(g):
        @pl.loop(0, chunks)
        def _(c):
            deposit_chunk(comp, push_comp, g * tiles + c * CHUNK_TILES, scales, loads, force_acc)

        @pl.when(g < GROUPS - 1)
        def _():
            arrived(push_recv, PER_GROUP, push_recv_sem.at[g + 1])
            pack(g + 1, push_recv, push_comp)

    flush = pltpu.make_async_copy(force_acc, force_out, out_sem)
    flush.start()
    arrived(got, DEVICES - 1, back_recv)
    got_out[...] = got[...]
    arrived(recv, DEVICES - 1, send_sem)
    arrived(recv, DEVICES - 1, push_send_sem)
    arrived(got, DEVICES - 1, back_send)
    flush.wait()


def finish(positions, got, slot, force_in, moved, out, table, force_acc, turned, in_sem, out_sem):
    ins, outs = [], []
    for k in range(3):
        part = pl.ds(k * NODES, NODES)
        ins.append(pltpu.make_async_copy(force_in.at[part], force_acc.at[part], in_sem.at[k]))
        outs.append(pltpu.make_async_copy(turned.at[k], out.at[k], out_sem.at[k]))
    for copy in ins:
        copy.start()
    for k in range(3):
        both = jnp.concatenate(
            [got[pl.ds(0, HALF, stride=2), k, :], got[pl.ds(1, HALF, stride=2), k, :]], axis=1
        )
        high, low = split(both)
        table[k * HALF:(k + 1) * HALF, :COLS] = high
        table[k * HALF:(k + 1) * HALF, COLS:] = low

    def one_row(r):
        p = slot[pl.ds(r, 1), :]
        low = one_hot(jnp.bitwise_and(p, 255), 256)
        hit = jnp.broadcast_to(lax.shift_right_logical(p, 8), (HALF, COLS)) == iota((HALF, COLS), 0)
        g = dot(table[...], jnp.concatenate([low, low], axis=0))
        for k in range(3):
            mine = jnp.sum(jnp.where(hit, g[k * HALF:(k + 1) * HALF], 0.0), axis=0, keepdims=True)
            moved[k, pl.ds(r, 1), :] = positions[k, pl.ds(r, 1), :] + time_step * mine

    pl.loop(0, EARLY, unroll=8)(one_row)
    for k in range(3):
        ins[k].wait()
        turned[k] = jnp.transpose(force_acc[k * NODES:(k + 1) * NODES])
        outs[k].start()
    pl.loop(EARLY, ROWS, unroll=8)(one_row)
    for copy in outs:
        copy.wait()


def local(velocity, positions, stiff_h, stiff_v, marker_owner, marker_element, marker_coords):
    markers = ROWS * COLS
    group_tiles = PER_GROUP * CAP // LANES
    vmem = pl.BlockSpec(memory_space=pltpu.VMEM)
    got, slot, force_acc = pl.pallas_call(
        step,
        out_shape=(
            jax.ShapeDtypeStruct((DEVICES, 4, LANES), F32),
            jax.ShapeDtypeStruct((ROWS, COLS), I32),
            jax.ShapeDtypeStruct((3 * NODES, ELEMS), F32),
        ),
        in_specs=[pl.BlockSpec(memory_space=pl.ANY)] * 7 + [vmem],
        out_specs=(vmem, vmem, pl.BlockSpec(memory_space=pl.ANY)),
        scratch_shapes=[
            pltpu.VMEM((3, ROWS, COLS), F32),
            pltpu.VMEM((ROWS, COLS), F32),
            pltpu.VMEM((ROWS, COLS), F32),
            pltpu.VMEM((1, markers), I32),
            pltpu.VMEM((1, markers), I32),
            pltpu.VMEM((3, markers), F32),
            pltpu.VMEM((3 * NODES, ELEMS), F32),
            pltpu.VMEM((4, ROWS + 16, COLS), F32),
            pltpu.VMEM((2, 4, 8, COLS), F32),
            pltpu.VMEM((6, ROWS, COLS), F32),
            pltpu.VMEM((7 * HALF, COLS), F32),
            pltpu.VMEM((DEVICES, 4, LANES), F32),
            pltpu.VMEM((DEVICES, 4, LANES), F32),
            pltpu.VMEM((DEVICES, 4, LANES), F32),
            pltpu.VMEM((DEVICES, 4, LANES), F32),
            pltpu.VMEM((TILES, 4, LANES), F32),
            pltpu.VMEM((TILES, 4, LANES), F32),
            pltpu.VMEM((group_tiles, 4, LANES), F32),
            pltpu.VMEM((DEVICES, 4, LANES), F32),
            pltpu.VMEM((DEVICES, 4, LANES), F32),
            pltpu.VMEM((3, ELEMS, NODES), F32),
            pltpu.VMEM((3 * NODES, 2 * ELEMS), BF),
            pltpu.VMEM((3 * NODES, 2 * CHUNK), BF),
            pltpu.SemaphoreType.DMA((6,)),
            pltpu.SemaphoreType.DMA,
            pltpu.SemaphoreType.DMA,
            pltpu.SemaphoreType.DMA((4,)),
            pltpu.SemaphoreType.DMA((4,)),
            pltpu.SemaphoreType.DMA,
            pltpu.SemaphoreType.DMA((GROUPS,)),
            pltpu.SemaphoreType.DMA,
            pltpu.SemaphoreType.DMA((GROUPS,)),
            pltpu.SemaphoreType.DMA,
            pltpu.SemaphoreType.DMA,
        ],
        compiler_params=pltpu.CompilerParams(collective_id=0, has_side_effects=True),
        name="step",
    )(
        positions, stiff_h, stiff_v,
        marker_owner.reshape(1, markers), marker_element.reshape(1, markers), marker_coords,
        velocity, jnp.asarray(SCALE_OF),
    )
    return pl.pallas_call(
        finish,
        out_shape=(
            jax.ShapeDtypeStruct((3, ROWS, COLS), F32),
            jax.ShapeDtypeStruct((3, ELEMS, NODES), F32),
        ),
        in_specs=[vmem] * 3 + [pl.BlockSpec(memory_space=pl.ANY)],
        out_specs=(vmem, pl.BlockSpec(memory_space=pl.ANY)),
        scratch_shapes=[
            pltpu.VMEM((3 * HALF, 2 * COLS), BF),
            pltpu.VMEM((3 * NODES, ELEMS), F32),
            pltpu.VMEM((3, ELEMS, NODES), F32),
            pltpu.SemaphoreType.DMA((3,)),
            pltpu.SemaphoreType.DMA((3,)),
        ],
        name="finish",
    )(positions, got, slot, force_acc)


def solution(mesh):
    return jax.shard_map(
        local,
        mesh=mesh,
        in_specs=(
            P(None, ("gx", "gy"), None),
            P(None, ("gx", "gy"), None),
            P(("gx", "gy"), None),
            P(("gx", "gy"), None),
            P(("gx", "gy"), None),
            P(("gx", "gy")),
            P(None, ("gx", "gy")),
        ),
        out_specs=(P(None, ("gx", "gy"), None), P(None, ("gx", "gy"), None)),
        check_vma=False,
    )
```
